32 devices in a mesh: leaf: 4 (over x, core), ctx: 8 (over z, y).
Axes of the slice: x: 2, y: 2, z: 4, core: 2. Of those that a mesh axis runs over, the one named last changes fastest.
Arguments:
- queries: bfloat16 [4096, 4096], P(('leaf', 'ctx')), parts along dimension 0, may hold values from -6 to 6
- keys: bfloat16 [4096, 512], P(('leaf', 'ctx')), parts along dimension 0, may hold values from -6 to 6
- values: bfloat16 [4096, 512], P(('leaf', 'ctx')), parts along dimension 0, may hold values from -6 to 6
- grad_out: bfloat16 [4096, 4096], P(('leaf', 'ctx')), parts along dimension 0, may hold values from -6 to 6
- block_path: int32 [32, 4], P('leaf'), parts along dimension 0, may hold values from -1 to 7, as said below
- assistant: int32 [4096], P(('leaf', 'ctx')), parts along dimension 0, may hold values from 0 to 1, as said below
Outputs:
- attention: bfloat16 [4096, 4096], P(('leaf', 'ctx')), parts along dimension 0
- grad_queries: bfloat16 [4096, 4096], P(('leaf', 'ctx')), parts along dimension 0
- grad_keys: bfloat16 [4096, 512], P(('leaf', 'ctx')), parts along dimension 0
- grad_values: bfloat16 [4096, 512], P(('leaf', 'ctx')), parts along dimension 0
The draws below stay inside these ranges and needn't reach their ends.
There are 4 independent parts, one for each index of `leaf`. The reference program is written for one: setup_inputs(seed, part) draws one part's arguments, and reference() takes and returns one part's arrays. A program takes and returns all parts, laid end to end along the dimension named above; each array names one. Nothing has to cross between parts.
Inputs may be any that keep to these rules, and one draw needn't show every extreme that they name: `block_path`: blocks lie in depth-first order of the tree; every node spans one block; block 0 is the root at depth 0. Row b holds at depth e <= depth(b) the block of b's ancestor node at that depth (b itself at e = depth(b)) and -1 below. `assistant`: each block of 128 tokens holds one run of ones.
All inputs are finite; a program needn't handle non-finite values.
Results may differ from the reference program's by a relative error of at most 0.0091.
Values may be sent and summed in bfloat16 or wider, within the bound.
No kernel may reach another device: no remote copies, remote signals or barrier semaphores. Data moves between devices by JAX's collectives and lax.ppermute only.
A program may use at most 128 MiB of HBM per device.

```python
import math
import jax
import jax.numpy as jnp
from jax import lax

TOK_DEV = 128
HQ = 32
KEY_HEADS = 4
HEAD_WIDTH = 128
HEADS_PER_KEY = 8
NBLK = 8
TREE_TOKENS = 1024


def tree_paths(key):
    block_keys = jax.random.split(jax.random.fold_in(key, 3), NBLK - 1)

    def advance(state, inputs):
        own_path, depth_now = state
        block_index, block_key = inputs
        highest = jnp.minimum(depth_now + 1, 3)
        depth_next = jax.random.randint(block_key, (), 1, highest + 1).astype(jnp.int32)
        tier_index = jnp.arange(4, dtype=jnp.int32)
        path_next = jnp.where(tier_index < depth_next, own_path, jnp.where(tier_index == depth_next, block_index, -1)).astype(jnp.int32)
        return ((path_next, depth_next), path_next)
    first_path = jnp.array([0, -1, -1, -1], dtype=jnp.int32)
    initial = (first_path, jnp.int32(0))
    _, rest_rows = lax.scan(advance, initial, (jnp.arange(1, NBLK, dtype=jnp.int32), block_keys))
    return jnp.concatenate([first_path[None, :], rest_rows], 0)


def draw_block_path(key, part):
    return tree_paths(key)


def draw_assistant(key, part):
    first_key, second_key = jax.random.split(jax.random.fold_in(key, 7))
    begin_at = jax.random.randint(first_key, (NBLK, 1), 0, TOK_DEV // 2)
    span_rows = jax.random.randint(second_key, (NBLK, 1), TOK_DEV // 4, TOK_DEV)
    offsets = jnp.arange(TOK_DEV)[None, :]
    inside = (offsets >= begin_at) & (offsets < begin_at + span_rows)
    return inside.astype(jnp.int32).reshape(-1)


def query_key_pair(key):
    base_key = jax.random.fold_in(key, 11)
    query_base, key_seed = jax.random.split(base_key, 2)
    query_draw = jnp.clip(jax.random.normal(query_base, (TREE_TOKENS, HQ * HEAD_WIDTH), jnp.float32), -6.0, 6.0)
    key_sample = jnp.clip(jax.random.normal(key_seed, (TREE_TOKENS, KEY_HEADS * HEAD_WIDTH), jnp.float32), -6.0, 6.0)
    return (query_draw, key_sample)


def draw_queries(key, part):
    return query_key_pair(key)[0].astype(jnp.bfloat16)


def draw_keys(key, part):
    return query_key_pair(key)[1].astype(jnp.bfloat16)


def level_of(rng, shape, cuts, least, largest):
    gain, own = 1.0, jax.random.fold_in(rng, 6)
    for dim, parts in cuts:
        steps = jnp.exp(jax.random.uniform(jax.random.fold_in(own, dim), (parts,), jnp.float32, least / len(cuts), largest / len(cuts)))
        gain = gain * jnp.repeat(steps, shape[dim] // parts).reshape([-1 if axis == dim else 1 for axis in range(len(shape))])
    return gain


def gaussian(key, dims, width, reach, pieces=(), kind=jnp.bfloat16):
    drawn = width * jax.random.normal(key, dims, jnp.float32)
    if pieces:
        drawn = drawn * level_of(key, dims, pieces, -0.22, 0.18)
    return jnp.clip(drawn, -reach, reach).astype(kind)


def setup_inputs(seed: int = 0, part: int = 0) -> dict:
    splits = jax.random.split(jax.random.key(seed), 7)
    part_keys = jax.random.split(jax.random.fold_in(splits[6], part), 7)
    queries = draw_queries(jax.random.fold_in(jax.random.fold_in(splits[6], part), 71), part)
    keys = draw_keys(jax.random.fold_in(jax.random.fold_in(splits[6], part), 71), part)
    values = gaussian(part_keys[2], (TREE_TOKENS, KEY_HEADS * HEAD_WIDTH), 1.0, 6.0, ((0, 8),))
    grad_out = gaussian(part_keys[3], (TREE_TOKENS, HQ * HEAD_WIDTH), 1.0, 6.0, ((0, 8),))
    block_path = draw_block_path(jax.random.fold_in(jax.random.fold_in(splits[6], part), 71), part)
    assistant = draw_assistant(jax.random.fold_in(jax.random.fold_in(splits[6], part), 71), part)
    return {"queries": queries, "keys": keys, "values": values, "grad_out": grad_out, "block_path": block_path, "assistant": assistant}


def attend_block(queries, grad_rows, slot_keys, slot_values, allowed):
    block_rows = queries.shape[0]
    head_cols = HEADS_PER_KEY * HEAD_WIDTH
    scaling = 1.0 / math.sqrt(HEAD_WIDTH)
    wide_mask = jnp.repeat(allowed, HEADS_PER_KEY, axis=0)
    attended_parts, query_parts, key_parts, value_parts = ([], [], [], [])
    for key_value_head in range(KEY_HEADS):
        query_matrix = queries[:, key_value_head * head_cols:(key_value_head + 1) * head_cols].reshape(block_rows * HEADS_PER_KEY, HEAD_WIDTH)
        grad_head = grad_rows[:, key_value_head * head_cols:(key_value_head + 1) * head_cols].reshape(block_rows * HEADS_PER_KEY, HEAD_WIDTH)
        key_cols = slot_keys[:, key_value_head * HEAD_WIDTH:(key_value_head + 1) * HEAD_WIDTH]
        value_cols = slot_values[:, key_value_head * HEAD_WIDTH:(key_value_head + 1) * HEAD_WIDTH]
        scores = jnp.dot(query_matrix, key_cols.T, preferred_element_type=jnp.float32) * scaling
        scores = jnp.where(wide_mask, scores, -jnp.inf)
        row_max = lax.optimization_barrier(jnp.max(scores, axis=1, keepdims=True))
        row_sum = lax.optimization_barrier(jnp.sum(jnp.exp(scores - row_max), axis=1, keepdims=True))
        weights = jnp.exp(scores - (row_max + jnp.log(row_sum)))
        rounded = weights.astype(jnp.bfloat16)
        attended = jnp.dot(rounded, value_cols, preferred_element_type=jnp.float32).astype(jnp.bfloat16)
        attended = lax.optimization_barrier(attended)
        row_delta = lax.optimization_barrier(jnp.sum(grad_head.astype(jnp.float32) * attended.astype(jnp.float32), axis=1, keepdims=True))
        grad_prob = jnp.dot(grad_head, value_cols.T, preferred_element_type=jnp.float32)
        grad_score = (weights * (grad_prob - row_delta)).astype(jnp.bfloat16)
        grad_query = (jnp.dot(grad_score, key_cols, preferred_element_type=jnp.float32) * scaling).astype(jnp.bfloat16)
        grad_key = jnp.dot(grad_score.T, query_matrix, preferred_element_type=jnp.float32) * scaling
        grad_value = jnp.dot(rounded.T, grad_head, preferred_element_type=jnp.float32)
        attended_parts.append(attended.reshape(block_rows, head_cols))
        query_parts.append(grad_query.reshape(block_rows, head_cols))
        key_parts.append(grad_key)
        value_parts.append(grad_value)
    return (jnp.concatenate(attended_parts, 1), jnp.concatenate(query_parts, 1), jnp.concatenate(key_parts, 1), jnp.concatenate(value_parts, 1))

def reference(queries, keys, values, grad_out, block_path, assistant):
    blocks = block_path.shape[0]
    block_rows = queries.shape[0] // blocks
    kv_width = keys.shape[1]
    depths = lax.optimization_barrier(jnp.sum((block_path >= 0).astype(jnp.int32), axis=1)) - 1
    key_blocks = keys.reshape(blocks, block_rows, kv_width)
    value_blocks = values.reshape(blocks, block_rows, kv_width)
    query_blocks = queries.reshape(blocks, block_rows, queries.shape[1])
    grad_rows = grad_out * assistant[:, None].astype(jnp.bfloat16)
    grad_blocks = grad_rows.reshape(blocks, block_rows, grad_out.shape[1])
    causal = jnp.arange(block_rows)[:, None] >= jnp.arange(block_rows)[None, :]

    def one_block(carried, block_index):
        key_total, value_total = carried
        own_path = block_path[block_index]
        own_depth = depths[block_index]
        slot_blocks = jnp.stack([own_path[0], own_path[1], own_path[2], block_index]).astype(jnp.int32)
        seen_slots = jnp.stack([own_depth > 0, own_depth > 1, own_depth > 2])
        clipped = jnp.clip(slot_blocks, 0, blocks - 1)
        slot_keys = key_blocks[clipped].reshape(4 * block_rows, kv_width)
        slot_values = value_blocks[clipped].reshape(4 * block_rows, kv_width)
        full_slots = jnp.repeat(seen_slots, block_rows)
        allowed = jnp.concatenate([jnp.broadcast_to(full_slots[None, :], (block_rows, 3 * block_rows)), causal], 1)
        attended, grad_query, grad_key, grad_value = attend_block(query_blocks[block_index], grad_blocks[block_index], slot_keys, slot_values, allowed)
        key_total = key_total.at[clipped].add(grad_key.reshape(4, block_rows, kv_width))
        value_total = value_total.at[clipped].add(grad_value.reshape(4, block_rows, kv_width))
        return ((key_total, value_total), (attended, grad_query))
    blank = jnp.zeros((blocks, block_rows, kv_width), jnp.float32)
    (key_total, value_total), (attended, grad_query) = lax.scan(one_block, (blank, blank), jnp.arange(blocks, dtype=jnp.int32))
    return (attended.reshape(-1, queries.shape[1]), grad_query.reshape(-1, queries.shape[1]), key_total.reshape(-1, kv_width).astype(jnp.bfloat16), value_total.reshape(-1, kv_width).astype(jnp.bfloat16))
```

```python
import functools
import math

import jax
import jax.numpy as jnp
from jax import lax
from jax.experimental import pallas as pl
from jax.experimental.pallas import tpu as pltpu
from jax.sharding import PartitionSpec as P

KEY_HEADS = 4
HEAD_WIDTH = 128
HEADS_PER_KEY = 8
FAR_SLOTS = 3
GROUP = KEY_HEADS
PAIR = 2
MASKED = -1e30
VMEM_LIMIT = 24 * 1024 * 1024


SMEM_SPEC = pl.BlockSpec(memory_space=pltpu.SMEM)
VMEM_SPEC = pl.BlockSpec(memory_space=pltpu.VMEM)
ANY_SPEC = pl.BlockSpec(memory_space=pl.ANY)


def wrap(x):
    return lax.rem(x + 2 * GROUP, GROUP)


def head_columns(head):
    return pl.ds(pl.multiple_of(head * HEAD_WIDTH, HEAD_WIDTH), HEAD_WIDTH)


def cost(flops, moved):
    return pl.CostEstimate(flops=flops, bytes_accessed=moved, transcendentals=0)


def pack_kernel(pos_ref, k_ref, v_ref, *outs):
    member = lax.rem(pos_ref[0], GROUP)
    for t in range(GROUP):
        cols = head_columns(wrap(member + t))
        outs[t][0] = k_ref[:, cols]
        outs[t][1] = v_ref[:, cols]


def select_kernel(count, pos_ref, path_ref, *refs):
    pieces, outs = refs[:count], refs[count : count + GROUP]
    held, in_sem, out_sem = refs[count + GROUP :]
    position = pos_ref[0]
    member, group = lax.rem(position, GROUP), lax.div(position, GROUP)
    loads = [
        pltpu.make_async_copy(pieces[i], held.at[i], in_sem.at[i]) for i in range(count)
    ]
    for copy in loads:
        copy.start()
    for copy in loads:
        copy.wait()
    stores = []
    for t in range(GROUP):
        block = group * GROUP + wrap(member + t)
        for e in range(FAR_SLOTS):
            ancestor = path_ref[block, e]
            seen = path_ref[block, e + 1] >= 0
            above = group - lax.div(ancestor, GROUP)
            index = above * GROUP + wrap(member - lax.rem(ancestor, GROUP))
            index = jnp.where(seen, index, 0)
            copy = pltpu.make_async_copy(
                held.at[index], outs[t].at[e], out_sem.at[t * FAR_SLOTS + e]
            )
            copy.start()
            stores.append(copy)
    for copy in stores:
        copy.wait()


def attend_kernel(rows, *refs):
    (pos_ref, path_ref, q_ref, go_ref, mask_ref, far_ref, k_ref, v_ref) = refs[:8]
    attn_ref, gq_ref, far_grad_ref, own_grad_ref = refs[-8:-4]
    bias, dk, dv, _ = refs[-4:]
    step = pl.program_id(0)
    scaling = 1.0 / math.sqrt(HEAD_WIDTH)
    position = pos_ref[0]
    seen = sum((path_ref[position, e + 1] >= 0).astype(jnp.int32) for e in range(FAR_SLOTS))
    far_cols = FAR_SLOTS * rows

    @pl.when(step == 0)
    def _():
        col = lax.broadcasted_iota(jnp.int32, bias.shape, 1)
        row = lax.broadcasted_iota(jnp.int32, bias.shape, 0)
        far = (col < far_cols) & (col < seen * rows)
        own = (col >= far_cols) & (col - far_cols <= row)
        bias[...] = jnp.where(far | own, 0.0, MASKED)
        dk[...] = jnp.zeros_like(dk)
        dv[...] = jnp.zeros_like(dv)

    kk = jnp.concatenate([far_ref[0, 0], far_ref[1, 0], far_ref[2, 0], k_ref[...]], 0)
    vv = jnp.concatenate([far_ref[0, 1], far_ref[1, 1], far_ref[2, 1], v_ref[...]], 0)
    mask = mask_ref[...]
    parts = [slice(i * HEAD_WIDTH, (i + 1) * HEAD_WIDTH) for i in range(PAIR)]
    qm = jnp.concatenate([q_ref[:, s] for s in parts], 0)
    gm = jnp.concatenate([go_ref[:, s] * mask for s in parts], 0)
    last = (((1,), (1,)), ((), ()))
    first = (((0,), (0,)), ((), ()))
    scores = lax.dot_general(qm, kk, last, preferred_element_type=jnp.float32)
    scores = scores * (scaling * math.log2(math.e)) + jnp.concatenate([bias[...]] * PAIR, 0)
    top = jnp.max(scores, axis=1, keepdims=True)
    weights = jnp.exp2(scores - top)
    total = jnp.sum(weights, axis=1, keepdims=True)
    weights = weights * (1.0 / total)
    rounded = weights.astype(jnp.bfloat16)
    attended = jnp.dot(rounded, vv, preferred_element_type=jnp.float32).astype(jnp.bfloat16)
    delta = jnp.sum(
        gm.astype(jnp.float32) * attended.astype(jnp.float32), axis=1, keepdims=True
    )
    grad_prob = lax.dot_general(gm, vv, last, preferred_element_type=jnp.float32)
    grad_score = (weights * (grad_prob - delta)).astype(jnp.bfloat16)
    grad_query = jnp.dot(grad_score, kk, preferred_element_type=jnp.float32) * scaling
    grad_query = grad_query.astype(jnp.bfloat16)
    for i, s in enumerate(parts):
        attn_ref[:, s] = attended[i * rows : (i + 1) * rows]
        gq_ref[:, s] = grad_query[i * rows : (i + 1) * rows]
    dk[...] += lax.dot_general(grad_score, qm, first, preferred_element_type=jnp.float32)
    dv[...] += lax.dot_general(rounded, gm, first, preferred_element_type=jnp.float32)

    @pl.when(step == pl.num_programs(0) - 1)
    def _():
        for e in range(FAR_SLOTS):
            s = slice(e * rows, (e + 1) * rows)
            far_grad_ref[e, 0] = (dk[s] * scaling).astype(jnp.bfloat16)
            far_grad_ref[e, 1] = dv[s].astype(jnp.bfloat16)
        own_grad_ref[0] = dk[far_cols:] * scaling
        own_grad_ref[1] = dv[far_cols:]


def attend(turn, scalars, queries, grad_out, mask, far, keys, values, before):
    rows, width = queries.shape
    steps = HEADS_PER_KEY // PAIR
    wide = PAIR * HEAD_WIDTH

    def head(pos):
        return wrap(lax.rem(pos[0], GROUP) - turn)

    wide_spec = pl.BlockSpec((rows, wide), lambda j, pos, path: (0, head(pos) * steps + j))
    head_spec = pl.BlockSpec((rows, HEAD_WIDTH), lambda j, pos, path: (0, head(pos)))
    mask_spec = pl.BlockSpec(mask.shape, lambda j, pos, path: (0, 0))
    far_spec = pl.BlockSpec(far.shape, lambda j, pos, path: (0, 0, 0, 0))
    own_spec = pl.BlockSpec((2, rows, HEAD_WIDTH), lambda j, pos, path: (0, 0, 0))
    inputs = [queries, grad_out, mask, far, keys, values]
    in_specs = [wide_spec, wide_spec, mask_spec, far_spec, head_spec, head_spec]
    aliases = {}
    if before is not None:
        aliases = {len(scalars) + len(inputs): 0, len(scalars) + len(inputs) + 1: 1}
        inputs += list(before)
        in_specs += [ANY_SPEC, ANY_SPEC]
    span = (FAR_SLOTS + 1) * rows
    return pl.pallas_call(
        functools.partial(attend_kernel, rows),
        grid_spec=pltpu.PrefetchScalarGridSpec(
            num_scalar_prefetch=len(scalars),
            grid=(steps,),
            in_specs=in_specs,
            out_specs=[wide_spec, wide_spec, far_spec, own_spec],
            scratch_shapes=[
                pltpu.VMEM((rows, span), jnp.float32),
                pltpu.VMEM((span, HEAD_WIDTH), jnp.float32),
                pltpu.VMEM((span, HEAD_WIDTH), jnp.float32),
                pltpu.SemaphoreType.DMA,
            ],
        ),
        out_shape=[
            jax.ShapeDtypeStruct(queries.shape, jnp.bfloat16),
            jax.ShapeDtypeStruct(queries.shape, jnp.bfloat16),
            jax.ShapeDtypeStruct(far.shape, jnp.bfloat16),
            jax.ShapeDtypeStruct((2, rows, HEAD_WIDTH), jnp.float32),
        ],
        input_output_aliases=aliases,
        cost_estimate=cost(12 * rows * HEADS_PER_KEY * span * HEAD_WIDTH, 8 * rows * wide * steps),
        compiler_params=pltpu.CompilerParams(vmem_limit_bytes=VMEM_LIMIT),
        name=f"attend_{turn}",
    )(*scalars, *inputs)


def reduce_kernel(count, pos_ref, path_ref, *refs):
    terms, outs, acc = refs[:GROUP], refs[GROUP : GROUP + count], refs[-1]
    position = pos_ref[0]
    member, group = lax.rem(position, GROUP), lax.div(position, GROUP)
    acc[...] = jnp.zeros_like(acc)
    for t in range(GROUP):
        block = group * GROUP + wrap(member + t)
        for e in range(FAR_SLOTS):
            ancestor = path_ref[block, e]
            above = group - lax.div(ancestor, GROUP)
            index = above * GROUP + wrap(lax.rem(ancestor, GROUP) - member)

            @pl.when(path_ref[block, e + 1] >= 0)
            def _(t=t, e=e, index=index):
                acc[index] += terms[t][e].astype(jnp.float32)

    for i in range(count):
        outs[i][...] = acc[i].astype(jnp.bfloat16)


def finish_kernel(pos_ref, *refs):
    own, pieces, gk_ref, gv_ref = refs[:GROUP], refs[GROUP:-2], refs[-2], refs[-1]
    member = lax.rem(pos_ref[0], GROUP)
    for t in range(GROUP):
        cols = head_columns(wrap(member - t))
        for part, out in enumerate((gk_ref, gv_ref)):
            total = own[t][part]
            for piece in pieces[t::GROUP]:
                total = total + piece[part].astype(jnp.float32)
            out[:, cols] = total.astype(jnp.bfloat16)


def small_call(kernel, name, in_specs, out_shape, out_spec, moved, scratch=()):
    return pl.pallas_call(
        kernel,
        in_specs=in_specs,
        out_specs=[out_spec] * len(out_shape),
        out_shape=out_shape,
        scratch_shapes=list(scratch),
        cost_estimate=cost(2 * moved, moved),
        compiler_params=pltpu.CompilerParams(vmem_limit_bytes=VMEM_LIMIT),
        name=name,
    )


def on_device(size, queries, keys, values, grad_out, block_path, assistant):
    rows = queries.shape[0]
    groups = size // GROUP
    pos = lax.axis_index("ctx").astype(jnp.int32).reshape(1)
    scalars = (pos, block_path)
    mask = jnp.broadcast_to(assistant[:, None].astype(jnp.bfloat16), (rows, HEAD_WIDTH))
    piece = jax.ShapeDtypeStruct((2, rows, HEAD_WIDTH), jnp.bfloat16)
    chosen = jax.ShapeDtypeStruct((FAR_SLOTS, 2, rows, HEAD_WIDTH), jnp.bfloat16)
    piece_bytes = 4 * rows * HEAD_WIDTH

    def inside(shift):
        return [(i, i - i % GROUP + (i + shift) % GROUP) for i in range(size)]

    def across(up, shift):
        pairs = []
        for i in range(size):
            group = i // GROUP + up
            if 0 <= group < groups:
                pairs.append((i, group * GROUP + (i + shift) % GROUP))
        return pairs

    def send(x, pairs):
        return lax.ppermute(x, "ctx", pairs)

    packed = small_call(
        pack_kernel, "pack", [SMEM_SPEC, VMEM_SPEC, VMEM_SPEC], [piece] * GROUP, VMEM_SPEC,
        8 * piece_bytes,
    )(pos, keys, values)
    far_pieces = [send(packed[t], across(d, t)) for d in range(1, groups) for t in range(GROUP)]
    near_pieces = [packed[0]] + [send(packed[t], inside(t)) for t in range(1, GROUP)]
    pieces = near_pieces + far_pieces

    picked = small_call(
        functools.partial(select_kernel, size), "select",
        [SMEM_SPEC, SMEM_SPEC] + [ANY_SPEC] * size, [chosen] * GROUP, ANY_SPEC,
        (size + 12) * piece_bytes,
        [
            pltpu.VMEM((size,) + piece.shape, jnp.bfloat16),
            pltpu.SemaphoreType.DMA((size,)),
            pltpu.SemaphoreType.DMA((GROUP * FAR_SLOTS,)),
        ],
    )(pos, block_path, *pieces)
    far = [picked[0]] + [send(picked[t], inside(t)) for t in range(1, GROUP)]

    before, far_grads, own_grads = None, [], []
    for t in range(GROUP):
        attention, grad_queries, far_grad, own_grad = attend(
            t, scalars, queries, grad_out, mask, far[t], keys, values, before
        )
        before = (attention, grad_queries)
        far_grads.append(far_grad if t == 0 else send(far_grad, inside(-t)))
        own_grads.append(own_grad)

    sums = small_call(
        functools.partial(reduce_kernel, size), "reduce",
        [SMEM_SPEC, SMEM_SPEC] + [VMEM_SPEC] * GROUP, [piece] * size, VMEM_SPEC,
        (size + 12) * piece_bytes,
        [pltpu.VMEM((size,) + piece.shape, jnp.float32)],
    )(pos, block_path, *far_grads)
    far_sums = [
        send(sums[d * GROUP + t], across(-d, t)) for d in range(1, groups) for t in range(GROUP)
    ]
    near_sums = [sums[0]] + [send(sums[t], inside(t)) for t in range(1, GROUP)]

    grad = jax.ShapeDtypeStruct(keys.shape, jnp.bfloat16)
    grad_keys, grad_values = small_call(
        finish_kernel, "finish", [SMEM_SPEC] + [VMEM_SPEC] * (GROUP + size), [grad, grad],
        VMEM_SPEC, (size + 12) * piece_bytes,
    )(pos, *own_grads, *near_sums, *far_sums)
    return attention, grad_queries, grad_keys, grad_values


def solution(mesh):
    tokens = P(("leaf", "ctx"))
    return jax.shard_map(
        functools.partial(on_device, mesh.shape["ctx"]),
        mesh=mesh,
        in_specs=(tokens, tokens, tokens, tokens, P("leaf"), tokens),
        out_specs=(tokens, tokens, tokens, tokens),
        check_vma=False,
    )
```

```python
import functools
import math

import jax
import jax.numpy as jnp
from jax import lax
from jax.experimental import pallas as pl
from jax.experimental.pallas import tpu as pltpu
from jax.sharding import PartitionSpec as P


KEY_HEADS = 4
HEAD_WIDTH = 128
HEADS_PER_KEY = 8
FAR_SLOTS = 3
GROUP = KEY_HEADS
MASKED = -1e30
VMEM_LIMIT = 24 * 1024 * 1024


SMEM_SPEC = pl.BlockSpec(memory_space=pltpu.SMEM)
VMEM_SPEC = pl.BlockSpec(memory_space=pltpu.VMEM)
HBM_SPEC = pl.BlockSpec(memory_space=pltpu.HBM)


def wrap(x):
    return lax.rem(x + 2 * GROUP, GROUP)


def head_columns(head):
    return pl.ds(pl.multiple_of(head * HEAD_WIDTH, HEAD_WIDTH), HEAD_WIDTH)


def cost(flops, moved):
    return pl.CostEstimate(flops=flops, bytes_accessed=moved, transcendentals=0)


def pack_kernel(pos_ref, k_ref, v_ref, *refs):
    outs, sem = refs[:GROUP], refs[-1]
    member = lax.rem(pos_ref[0], GROUP)
    copies = []
    for t in range(GROUP):
        cols = head_columns(wrap(member + t))
        for part, source in enumerate((k_ref, v_ref)):
            copies.append(
                pltpu.make_async_copy(source.at[:, cols], outs[t].at[part], sem.at[2 * t + part])
            )
    for copy in copies:
        copy.start()
    for copy in copies:
        copy.wait()


def select_kernel(count, pos_ref, path_ref, *refs):
    pieces, outs, held = refs[:count], refs[count : count + GROUP], refs[-1]
    position = pos_ref[0]
    member, group = lax.rem(position, GROUP), lax.div(position, GROUP)
    for i in range(count):
        held[i] = pieces[i][...]
    for t in range(GROUP):
        block = group * GROUP + wrap(member + t)
        for e in range(FAR_SLOTS):
            ancestor = path_ref[block, e]
            seen = path_ref[block, e + 1] >= 0
            above = group - lax.div(ancestor, GROUP)
            index = above * GROUP + wrap(member - lax.rem(ancestor, GROUP))
            outs[t][e] = held[jnp.where(seen, index, 0)]


def stage_kernel(mask_ref, q_hbm, go_hbm, q_ref, gm_ref, sem):
    copies = [
        pltpu.make_async_copy(q_hbm, q_ref, sem.at[0]),
        pltpu.make_async_copy(go_hbm, gm_ref, sem.at[1]),
    ]
    for copy in copies:
        copy.start()
    for copy in copies:
        copy.wait()
    mask = mask_ref[...]
    for i in range(gm_ref.shape[1] // HEAD_WIDTH):
        cols = slice(i * HEAD_WIDTH, (i + 1) * HEAD_WIDTH)
        gm_ref[:, cols] = gm_ref[:, cols] * mask


def attend_kernel(turn, rows, *refs):
    (pos_ref, path_ref, q_ref, gm_ref, far_ref, own_ref) = refs[:6]
    attn_ref, gq_ref, far_grad_ref, own_grad_ref = refs[6:]
    scaling = 1.0 / math.sqrt(HEAD_WIDTH)
    position = pos_ref[0]
    head = wrap(lax.rem(position, GROUP) - turn)
    far_rows = FAR_SLOTS * rows
    last = (((1,), (1,)), ((), ()))
    first = (((0,), (0,)), ((), ()))

    def dot(left, right, dims=(((1,), (0,)), ((), ()))):
        return lax.dot_general(left, right, dims, preferred_element_type=jnp.float32)

    def rows_of(ref):
        parts = [
            ref[:, head_columns(head * HEADS_PER_KEY + i)] for i in range(HEADS_PER_KEY)
        ]
        return jnp.concatenate(parts, 0)

    kk = jnp.concatenate([far_ref[e, 0] for e in range(FAR_SLOTS)] + [own_ref[0]], 0)
    vv = jnp.concatenate([far_ref[e, 1] for e in range(FAR_SLOTS)] + [own_ref[1]], 0)
    qm, gm = rows_of(q_ref), rows_of(gm_ref)
    key = lax.broadcasted_iota(jnp.int32, (rows, rows), 0)
    token = lax.broadcasted_iota(jnp.int32, (rows, rows), 1)
    causal = jnp.where(key <= token, 0.0, MASKED)
    scores = dot(kk, qm, last)
    parts = [
        scores[e * rows : (e + 1) * rows] + jnp.where(path_ref[position, e + 1] >= 0, 0.0, MASKED)
        for e in range(FAR_SLOTS)
    ]
    parts.append(scores[far_rows:] + jnp.concatenate([causal] * HEADS_PER_KEY, 1))
    scores = jnp.concatenate(parts, 0)
    top = jnp.max(scores, axis=0, keepdims=True)
    weights = jnp.exp2((scores - top) * (scaling * math.log2(math.e)))
    weights = weights * (1.0 / jnp.sum(weights, axis=0, keepdims=True))
    rounded = weights.astype(jnp.bfloat16)
    grad_prob = dot(vv, gm, last)
    delta = jnp.sum(weights * grad_prob, axis=0, keepdims=True)
    grad_score = (weights * (grad_prob - delta)).astype(jnp.bfloat16)
    attended = dot(vv, rounded, first)
    grad_query = dot(kk, grad_score, first) * scaling
    for i in range(HEADS_PER_KEY):
        s = slice(i * rows, (i + 1) * rows)
        cols = slice(i * HEAD_WIDTH, (i + 1) * HEAD_WIDTH)
        attn_ref[:, cols] = attended[:, s].T.astype(jnp.bfloat16)
        gq_ref[:, cols] = grad_query[:, s].T.astype(jnp.bfloat16)
    grad_key = dot(grad_score, qm) * scaling
    grad_value = dot(rounded, gm)
    for e in range(FAR_SLOTS):
        s = slice(e * rows, (e + 1) * rows)
        far_grad_ref[e, 0] = grad_key[s].astype(jnp.bfloat16)
        far_grad_ref[e, 1] = grad_value[s].astype(jnp.bfloat16)
    own_grad_ref[0] = grad_key[far_rows:]
    own_grad_ref[1] = grad_value[far_rows:]


def attend(turn, pos, path, queries, grad_rows, far, own):
    rows = queries.shape[0]
    width = HEADS_PER_KEY * HEAD_WIDTH
    block = jax.ShapeDtypeStruct((rows, width), jnp.bfloat16)
    span = (FAR_SLOTS + 1) * rows
    return pl.pallas_call(
        functools.partial(attend_kernel, turn, rows),
        in_specs=[SMEM_SPEC] * 2 + [VMEM_SPEC] * 4,
        out_specs=[VMEM_SPEC] * 4,
        out_shape=[
            block,
            block,
            jax.ShapeDtypeStruct(far.shape, jnp.bfloat16),
            jax.ShapeDtypeStruct(own.shape, jnp.float32),
        ],
        cost_estimate=cost(12 * rows * HEADS_PER_KEY * span * HEAD_WIDTH, 8 * rows * width),
        compiler_params=pltpu.CompilerParams(vmem_limit_bytes=VMEM_LIMIT),
    )(pos, path, queries, grad_rows, far, own)


def store_kernel(pos_ref, *refs):
    blocks, outs, sem = refs[: 2 * GROUP], refs[2 * GROUP : -1], refs[-1]
    width = HEADS_PER_KEY * HEAD_WIDTH
    member = lax.rem(pos_ref[0], GROUP)
    copies = []
    for t in range(GROUP):
        head = wrap(member - t)
        cols = pl.ds(pl.multiple_of(head * width, width), width)
        for part in range(2):
            i = 2 * t + part
            copies.append(pltpu.make_async_copy(blocks[i], outs[part].at[:, cols], sem.at[i]))
    for copy in copies:
        copy.start()
    for copy in copies:
        copy.wait()


def reduce_kernel(count, pos_ref, path_ref, *refs):
    terms, outs, acc = refs[:GROUP], refs[GROUP : GROUP + count], refs[-1]
    position = pos_ref[0]
    member, group = lax.rem(position, GROUP), lax.div(position, GROUP)
    acc[...] = jnp.zeros_like(acc)
    for t in range(GROUP):
        block = group * GROUP + wrap(member + t)
        for e in range(FAR_SLOTS):
            ancestor = path_ref[block, e]
            above = group - lax.div(ancestor, GROUP)
            index = above * GROUP + wrap(lax.rem(ancestor, GROUP) - member)

            @pl.when(path_ref[block, e + 1] >= 0)
            def _(t=t, e=e, index=index):
                acc[index] += terms[t][e].astype(jnp.float32)

    for i in range(count):
        outs[i][...] = acc[i].astype(jnp.bfloat16)


def finish_kernel(pos_ref, *refs):
    own, pieces, gk_ref, gv_ref = refs[:GROUP], refs[GROUP:-2], refs[-2], refs[-1]
    member = lax.rem(pos_ref[0], GROUP)
    for t in range(GROUP):
        cols = head_columns(wrap(member - t))
        for part, out in enumerate((gk_ref, gv_ref)):
            total = own[t][part]
            for piece in pieces[t::GROUP]:
                total = total + piece[part].astype(jnp.float32)
            out[:, cols] = total.astype(jnp.bfloat16)


def small_call(kernel, in_specs, out_specs, out_shape, moved, scratch=()):
    return pl.pallas_call(
        kernel,
        in_specs=in_specs,
        out_specs=out_specs,
        out_shape=out_shape,
        scratch_shapes=list(scratch),
        cost_estimate=cost(2 * moved, moved),
        compiler_params=pltpu.CompilerParams(vmem_limit_bytes=VMEM_LIMIT),
    )


def on_device(size, queries, keys, values, grad_out, block_path, assistant):
    rows = queries.shape[0]
    groups = size // GROUP
    pos = lax.axis_index("ctx").astype(jnp.int32).reshape(1)
    mask = jnp.broadcast_to(assistant[:, None].astype(jnp.bfloat16), (rows, HEAD_WIDTH))
    piece = jax.ShapeDtypeStruct((2, rows, HEAD_WIDTH), jnp.bfloat16)
    chosen = jax.ShapeDtypeStruct((FAR_SLOTS, 2, rows, HEAD_WIDTH), jnp.bfloat16)
    wide = jax.ShapeDtypeStruct(queries.shape, jnp.bfloat16)
    piece_bytes = 4 * rows * HEAD_WIDTH

    def inside(shift):
        return [(i, i - i % GROUP + (i + shift) % GROUP) for i in range(size)]

    def across(up, shift):
        pairs = []
        for i in range(size):
            group = i // GROUP + up
            if 0 <= group < groups:
                pairs.append((i, group * GROUP + (i + shift) % GROUP))
        return pairs

    def send(x, pairs):
        return lax.ppermute(x, "ctx", pairs)

    def far_sends(parts, sign):
        return [
            send(parts[(d * GROUP + t) % len(parts)], across(sign * d, t))
            for d in range(1, groups)
            for t in range(GROUP)
        ]

    def near_sends(parts, sign=1):
        return [parts[0]] + [send(parts[t], inside(sign * t)) for t in range(1, GROUP)]

    packed = small_call(
        pack_kernel, [SMEM_SPEC, HBM_SPEC, HBM_SPEC], [VMEM_SPEC] * GROUP,
        [piece] * GROUP, 8 * piece_bytes, [pltpu.SemaphoreType.DMA((2 * GROUP,))],
    )(pos, keys, values)
    far_pieces = far_sends(packed, 1)
    pieces = near_sends(packed) + far_pieces

    staged, grad_rows = small_call(
        stage_kernel, [VMEM_SPEC, HBM_SPEC, HBM_SPEC], [VMEM_SPEC] * 2, [wide] * 2,
        32 * piece_bytes, [pltpu.SemaphoreType.DMA((2,))],
    )(mask, queries, grad_out)

    picked = small_call(
        functools.partial(select_kernel, size),
        [SMEM_SPEC, SMEM_SPEC] + [VMEM_SPEC] * size, [VMEM_SPEC] * GROUP, [chosen] * GROUP,
        (size + 12) * piece_bytes, [pltpu.VMEM((size,) + piece.shape, jnp.bfloat16)],
    )(pos, block_path, *pieces)
    far = near_sends(picked)

    blocks, far_grads, own_grads = [], [], []
    for t in range(GROUP):
        attended, grad_query, far_grad, own_grad = attend(
            t, pos, block_path, staged, grad_rows, far[t], packed[-t % GROUP]
        )
        blocks += [attended, grad_query]
        far_grads.append(far_grad)
        own_grads.append(own_grad)
    far_grads = near_sends(far_grads, -1)

    attention, grad_queries = small_call(
        store_kernel, [SMEM_SPEC] + [VMEM_SPEC] * (2 * GROUP), [HBM_SPEC] * 2,
        [wide] * 2, 32 * piece_bytes, [pltpu.SemaphoreType.DMA((2 * GROUP,))],
    )(pos, *blocks)

    sums = small_call(
        functools.partial(reduce_kernel, size),
        [SMEM_SPEC, SMEM_SPEC] + [VMEM_SPEC] * GROUP, [VMEM_SPEC] * size, [piece] * size,
        (size + 12) * piece_bytes, [pltpu.VMEM((size,) + piece.shape, jnp.float32)],
    )(pos, block_path, *far_grads)
    far_sums = far_sends(sums, -1)
    near_sums = near_sends(sums[:GROUP])

    grad = jax.ShapeDtypeStruct(keys.shape, jnp.bfloat16)
    grad_keys, grad_values = small_call(
        finish_kernel, [SMEM_SPEC] + [VMEM_SPEC] * (GROUP + size), [VMEM_SPEC] * 2,
        [grad, grad], (size + 12) * piece_bytes,
    )(pos, *own_grads, *near_sums, *far_sums)
    return attention, grad_queries, grad_keys, grad_values


def solution(mesh):
    tokens = P(("leaf", "ctx"))

    def body(*args):
        return on_device(mesh.shape["ctx"], *args)

    return jax.shard_map(
        body,
        mesh=mesh,
        in_specs=(tokens, tokens, tokens, tokens, P("leaf"), tokens),
        out_specs=(tokens, tokens, tokens, tokens),
        check_vma=False,
    )
```

```python
import functools
import math

import jax
import jax.numpy as jnp
from jax import lax
from jax.experimental import pallas as pl
from jax.experimental.pallas import tpu as pltpu
from jax.sharding import PartitionSpec as P


KEY_HEADS = 4
HEAD_WIDTH = 128
HEADS_PER_KEY = 8
FAR_SLOTS = 3
GROUP = KEY_HEADS
MASKED = -1e30
COVER_FLOPS = 4_000_000_000
VMEM_LIMIT = 24 * 1024 * 1024


SMEM_SPEC = pl.BlockSpec(memory_space=pltpu.SMEM)
VMEM_SPEC = pl.BlockSpec(memory_space=pltpu.VMEM)
HBM_SPEC = pl.BlockSpec(memory_space=pltpu.HBM)


LAST = (((1,), (1,)), ((), ()))
FIRST = (((0,), (0,)), ((), ()))
SCALING = 1.0 / math.sqrt(HEAD_WIDTH)


def dot(left, right, dims=(((1,), (0,)), ((), ()))):
    return lax.dot_general(left, right, dims, preferred_element_type=jnp.float32)


def stack_slots(far_ref, own_ref, part):
    return jnp.concatenate([far_ref[e, part] for e in range(FAR_SLOTS)] + [own_ref[part]], 0)


def wrap(x):
    return lax.rem(x + 2 * GROUP, GROUP)


def head_columns(head):
    return pl.ds(pl.multiple_of(head * HEAD_WIDTH, HEAD_WIDTH), HEAD_WIDTH)


def cost(flops, moved):
    return pl.CostEstimate(flops=flops, bytes_accessed=moved, transcendentals=0)


def pack_kernel(pos_ref, k_ref, v_ref, *refs):
    outs, sem = refs[:GROUP], refs[-1]
    member = lax.rem(pos_ref[0], GROUP)
    copies = []
    for t in range(GROUP):
        cols = head_columns(wrap(member + t))
        for part, source in enumerate((k_ref, v_ref)):
            copies.append(
                pltpu.make_async_copy(source.at[:, cols], outs[t].at[part], sem.at[2 * t + part])
            )
    for copy in copies:
        copy.start()
    for copy in copies:
        copy.wait()


def select_kernel(count, pos_ref, path_ref, *refs):
    pieces, outs, held = refs[:count], refs[count : count + GROUP], refs[-1]
    position = pos_ref[0]
    member, group = lax.rem(position, GROUP), lax.div(position, GROUP)
    for i in range(count):
        held[i] = pieces[i][...]
    for t in range(GROUP):
        block = group * GROUP + wrap(member + t)
        for e in range(FAR_SLOTS):
            ancestor = path_ref[block, e]
            seen = path_ref[block, e + 1] >= 0
            above = group - lax.div(ancestor, GROUP)
            index = above * GROUP + wrap(member - lax.rem(ancestor, GROUP))
            outs[t][e] = held[jnp.where(seen, index, 0)]


def attend_kernel(turn, rows, *refs):
    (pos_ref, path_ref, mask_ref, q_ref, go_ref, far_ref, own_ref) = refs[:7]
    weights_ref, grad_score_ref, far_grad_ref, own_grad_ref = refs[7:]
    position = pos_ref[0]
    head = wrap(lax.rem(position, GROUP) - turn)
    far_rows = FAR_SLOTS * rows
    mask = mask_ref[...]
    blocks = [head_columns(head * HEADS_PER_KEY + i) for i in range(HEADS_PER_KEY)]
    kk, vv = stack_slots(far_ref, own_ref, 0), stack_slots(far_ref, own_ref, 1)
    qm = jnp.concatenate([q_ref[:, cols] for cols in blocks], 0)
    gm = jnp.concatenate([go_ref[:, cols] * mask for cols in blocks], 0)
    key = lax.broadcasted_iota(jnp.int32, (rows, rows), 0)
    token = lax.broadcasted_iota(jnp.int32, (rows, rows), 1)
    causal = jnp.where(key <= token, 0.0, MASKED)
    scores = dot(kk, qm, LAST)
    parts = [
        scores[e * rows : (e + 1) * rows] + jnp.where(path_ref[position, e + 1] >= 0, 0.0, MASKED)
        for e in range(FAR_SLOTS)
    ]
    parts.append(scores[far_rows:] + jnp.concatenate([causal] * HEADS_PER_KEY, 1))
    scores = jnp.concatenate(parts, 0)
    top = jnp.max(scores, axis=0, keepdims=True)
    weights = jnp.exp2((scores - top) * (SCALING * math.log2(math.e)))
    weights = weights * (1.0 / jnp.sum(weights, axis=0, keepdims=True))
    rounded = weights.astype(jnp.bfloat16)
    grad_prob = dot(vv, gm, LAST)
    delta = jnp.sum(weights * grad_prob, axis=0, keepdims=True)
    grad_score = (weights * (grad_prob - delta)).astype(jnp.bfloat16)
    weights_ref[...] = rounded
    grad_score_ref[...] = grad_score
    grad_key = dot(grad_score, qm) * SCALING
    grad_value = dot(rounded, gm)
    for e in range(FAR_SLOTS):
        s = slice(e * rows, (e + 1) * rows)
        far_grad_ref[e, 0] = grad_key[s].astype(jnp.bfloat16)
        far_grad_ref[e, 1] = grad_value[s].astype(jnp.bfloat16)
    own_grad_ref[0] = grad_key[far_rows:]
    own_grad_ref[1] = grad_value[far_rows:]


def output_kernel(rows, *refs):
    weights_ref, grad_score_ref, far_ref, own_ref, attn_ref, gq_ref = refs
    kk, vv = stack_slots(far_ref, own_ref, 0), stack_slots(far_ref, own_ref, 1)
    attended = dot(vv, weights_ref[...], FIRST)
    grad_query = dot(kk, grad_score_ref[...], FIRST) * SCALING
    for i in range(HEADS_PER_KEY):
        s = slice(i * rows, (i + 1) * rows)
        cols = slice(i * HEAD_WIDTH, (i + 1) * HEAD_WIDTH)
        attn_ref[:, cols] = attended[:, s].T.astype(jnp.bfloat16)
        gq_ref[:, cols] = grad_query[:, s].T.astype(jnp.bfloat16)


def attend(turn, pos, path, mask, queries, grad_out, far, own):
    rows = queries.shape[0]
    span = (FAR_SLOTS + 1) * rows
    pairs = rows * HEADS_PER_KEY * span
    square = jax.ShapeDtypeStruct((span, HEADS_PER_KEY * rows), jnp.bfloat16)
    return pl.pallas_call(
        functools.partial(attend_kernel, turn, rows),
        in_specs=[SMEM_SPEC] * 2 + [VMEM_SPEC] * 5,
        out_specs=[VMEM_SPEC] * 4,
        out_shape=[
            square,
            square,
            jax.ShapeDtypeStruct(far.shape, jnp.bfloat16),
            jax.ShapeDtypeStruct(own.shape, jnp.float32),
        ],
        cost_estimate=cost(8 * pairs * HEAD_WIDTH, 8 * pairs),
        compiler_params=pltpu.CompilerParams(vmem_limit_bytes=VMEM_LIMIT),
    )(pos, path, mask, queries, grad_out, far, own)


def output(weights, grad_score, far, own):
    rows = own.shape[1]
    block = jax.ShapeDtypeStruct((rows, HEADS_PER_KEY * HEAD_WIDTH), jnp.bfloat16)
    return pl.pallas_call(
        functools.partial(output_kernel, rows),
        in_specs=[VMEM_SPEC] * 4,
        out_specs=[VMEM_SPEC] * 2,
        out_shape=[block, block],
        cost_estimate=cost(4 * weights.size * HEAD_WIDTH, 4 * weights.size),
        compiler_params=pltpu.CompilerParams(vmem_limit_bytes=VMEM_LIMIT),
    )(weights, grad_score, far, own)


def store_kernel(pos_ref, *refs):
    blocks, outs, sem = refs[: 2 * GROUP], refs[2 * GROUP : -1], refs[-1]
    width = HEADS_PER_KEY * HEAD_WIDTH
    member = lax.rem(pos_ref[0], GROUP)
    copies = []
    for t in range(GROUP):
        head = wrap(member - t)
        cols = pl.ds(pl.multiple_of(head * width, width), width)
        for part in range(2):
            i = 2 * t + part
            copies.append(pltpu.make_async_copy(blocks[i], outs[part].at[:, cols], sem.at[i]))
    for copy in copies:
        copy.start()
    for copy in copies:
        copy.wait()


def reduce_kernel(count, pos_ref, path_ref, *refs):
    terms, outs, acc = refs[:GROUP], refs[GROUP : GROUP + count], refs[-1]
    position = pos_ref[0]
    member, group = lax.rem(position, GROUP), lax.div(position, GROUP)
    acc[...] = jnp.zeros_like(acc)
    for t in range(GROUP):
        block = group * GROUP + wrap(member + t)
        for e in range(FAR_SLOTS):
            ancestor = path_ref[block, e]
            above = group - lax.div(ancestor, GROUP)
            index = above * GROUP + wrap(lax.rem(ancestor, GROUP) - member)

            @pl.when(path_ref[block, e + 1] >= 0)
            def _(t=t, e=e, index=index):
                acc[index] += terms[t][e].astype(jnp.float32)

    for i in range(count):
        outs[i][...] = acc[i].astype(jnp.bfloat16)


def finish_kernel(pos_ref, *refs):
    own, pieces, gk_ref, gv_ref = refs[:GROUP], refs[GROUP:-2], refs[-2], refs[-1]
    member = lax.rem(pos_ref[0], GROUP)
    for t in range(GROUP):
        cols = head_columns(wrap(member - t))
        for part, out in enumerate((gk_ref, gv_ref)):
            total = own[t][part]
            for piece in pieces[t::GROUP]:
                total = total + piece[part].astype(jnp.float32)
            out[:, cols] = total.astype(jnp.bfloat16)


def small_call(kernel, in_specs, out_specs, out_shape, moved, scratch=(), flops=0):
    return pl.pallas_call(
        kernel,
        in_specs=in_specs,
        out_specs=out_specs,
        out_shape=out_shape,
        scratch_shapes=list(scratch),
        cost_estimate=cost(flops or 2 * moved, moved),
        compiler_params=pltpu.CompilerParams(vmem_limit_bytes=VMEM_LIMIT),
    )


def on_device(size, queries, keys, values, grad_out, block_path, assistant):
    rows = queries.shape[0]
    groups = size // GROUP
    pos = lax.axis_index("ctx").astype(jnp.int32).reshape(1)
    mask = jnp.broadcast_to(assistant[:, None].astype(jnp.bfloat16), (rows, HEAD_WIDTH))
    piece = jax.ShapeDtypeStruct((2, rows, HEAD_WIDTH), jnp.bfloat16)
    chosen = jax.ShapeDtypeStruct((FAR_SLOTS, 2, rows, HEAD_WIDTH), jnp.bfloat16)
    wide = jax.ShapeDtypeStruct(queries.shape, jnp.bfloat16)
    piece_bytes = 4 * rows * HEAD_WIDTH

    def inside(shift):
        return [(i, i - i % GROUP + (i + shift) % GROUP) for i in range(size)]

    def across(up, shift):
        pairs = []
        for i in range(size):
            group = i // GROUP + up
            if 0 <= group < groups:
                pairs.append((i, group * GROUP + (i + shift) % GROUP))
        return pairs

    def send(x, pairs):
        return lax.ppermute(x, "ctx", pairs)

    def far_sends(parts, sign):
        return [
            send(parts[(d * GROUP + t) % len(parts)], across(sign * d, t))
            for d in range(1, groups)
            for t in range(GROUP)
        ]

    def near_sends(parts, sign=1):
        return [parts[0]] + [send(parts[t], inside(sign * t)) for t in range(1, GROUP)]

    packed = small_call(
        pack_kernel, [SMEM_SPEC, HBM_SPEC, HBM_SPEC], [VMEM_SPEC] * GROUP,
        [piece] * GROUP, 8 * piece_bytes, [pltpu.SemaphoreType.DMA((2 * GROUP,))],
    )(pos, *(pltpu.with_memory_space_constraint(x, pltpu.HBM) for x in (keys, values)))
    far_pieces = far_sends(packed, 1)
    pieces = near_sends(packed) + far_pieces

    picked = small_call(
        functools.partial(select_kernel, size),
        [SMEM_SPEC, SMEM_SPEC] + [VMEM_SPEC] * size, [VMEM_SPEC] * GROUP, [chosen] * GROUP,
        (size + 12) * piece_bytes, [pltpu.VMEM((size,) + piece.shape, jnp.bfloat16)],
        COVER_FLOPS,
    )(pos, block_path, *pieces)
    far = near_sends(picked)

    blocks, far_grads, own_grads = [], [], []
    for t in range(GROUP):
        weights, grad_score, far_grad, own_grad = attend(
            t, pos, block_path, mask, queries, grad_out, far[t], packed[-t % GROUP]
        )
        blocks += output(weights, grad_score, far[t], packed[-t % GROUP])
        far_grads.append(far_grad)
        own_grads.append(own_grad)
    far_grads = near_sends(far_grads, -1)

    attention, grad_queries = small_call(
        store_kernel, [SMEM_SPEC] + [VMEM_SPEC] * (2 * GROUP), [HBM_SPEC] * 2,
        [wide] * 2, 32 * piece_bytes, [pltpu.SemaphoreType.DMA((2 * GROUP,))],
    )(pos, *blocks)

    sums = small_call(
        functools.partial(reduce_kernel, size),
        [SMEM_SPEC, SMEM_SPEC] + [VMEM_SPEC] * GROUP, [VMEM_SPEC] * size, [piece] * size,
        (size + 12) * piece_bytes, [pltpu.VMEM((size,) + piece.shape, jnp.float32)],
    )(pos, block_path, *far_grads)
    far_sums = far_sends(sums, -1)
    near_sums = near_sends(sums[:GROUP])

    grad = jax.ShapeDtypeStruct(keys.shape, jnp.bfloat16)
    grad_keys, grad_values = small_call(
        finish_kernel, [SMEM_SPEC] + [VMEM_SPEC] * (GROUP + size), [VMEM_SPEC] * 2,
        [grad, grad], (size + 12) * piece_bytes,
    )(pos, *own_grads, *near_sums, *far_sums)
    return attention, grad_queries, grad_keys, grad_values


def solution(mesh):
    tokens = P(("leaf", "ctx"))

    def body(*args):
        return on_device(mesh.shape["ctx"], *args)

    return jax.shard_map(
        body,
        mesh=mesh,
        in_specs=(tokens, tokens, tokens, tokens, P("leaf"), tokens),
        out_specs=(tokens, tokens, tokens, tokens),
        check_vma=False,
    )
```

```python
import functools
import math

import jax
import jax.numpy as jnp
from jax import lax
from jax.experimental import pallas as pl
from jax.experimental.pallas import tpu as pltpu
from jax.sharding import PartitionSpec as P


KEY_HEADS = 4
HEAD_WIDTH = 128
HEADS_PER_KEY = 8
FAR_SLOTS = 3
GROUP = KEY_HEADS
MASKED = -1e30
COVER_FLOPS = 4_000_000_000
VMEM_LIMIT = 24 * 1024 * 1024


SMEM_SPEC = pl.BlockSpec(memory_space=pltpu.SMEM)
VMEM_SPEC = pl.BlockSpec(memory_space=pltpu.VMEM)
HBM_SPEC = pl.BlockSpec(memory_space=pltpu.HBM)


LAST = (((1,), (1,)), ((), ()))
FIRST = (((0,), (0,)), ((), ()))
SCALING = 1.0 / math.sqrt(HEAD_WIDTH)


def dot(left, right, dims=(((1,), (0,)), ((), ()))):
    return lax.dot_general(left, right, dims, preferred_element_type=jnp.float32)


def stack_slots(far_ref, own_ref, part):
    return jnp.concatenate([far_ref[e, part] for e in range(FAR_SLOTS)] + [own_ref[part]], 0)


def head_columns(head):
    return pl.ds(pl.multiple_of(head * HEAD_WIDTH, HEAD_WIDTH), HEAD_WIDTH)


def cost(flops, moved):
    return pl.CostEstimate(flops=flops, bytes_accessed=moved, transcendentals=0)


def pack_kernel(pos_ref, k_ref, v_ref, *refs):
    outs, sem = refs[:GROUP], refs[-1]
    member = lax.rem(pos_ref[0], GROUP)
    copies = []
    for t in range(GROUP):
        cols = head_columns(member ^ t)
        for part, source in enumerate((k_ref, v_ref)):
            copies.append(
                pltpu.make_async_copy(source.at[:, cols], outs[t].at[part], sem.at[2 * t + part])
            )
    for copy in copies:
        copy.start()
    for copy in copies:
        copy.wait()


def select_kernel(count, pos_ref, path_ref, *refs):
    pieces, outs, held = refs[:count], refs[count : count + GROUP], refs[-1]
    position = pos_ref[0]
    member, group = lax.rem(position, GROUP), lax.div(position, GROUP)
    for i in range(count):
        held[i] = pieces[i][...]
    for t in range(GROUP):
        block = group * GROUP + member ^ t
        for e in range(FAR_SLOTS):
            ancestor = path_ref[block, e]
            seen = path_ref[block, e + 1] >= 0
            above = group - lax.div(ancestor, GROUP)
            index = above * GROUP + (member ^ lax.rem(ancestor, GROUP))
            outs[t][e] = held[jnp.where(seen, index, 0)]


def attend_kernel(turn, rows, *refs):
    (pos_ref, path_ref, mask_ref, q_ref, go_ref, far_ref, own_ref) = refs[:7]
    weights_ref, grad_score_ref, far_grad_ref, own_grad_ref = refs[7:]
    position = pos_ref[0]
    head = lax.rem(position, GROUP) ^ turn
    far_rows = FAR_SLOTS * rows
    mask = mask_ref[...]
    blocks = [head_columns(head * HEADS_PER_KEY + i) for i in range(HEADS_PER_KEY)]
    kk, vv = stack_slots(far_ref, own_ref, 0), stack_slots(far_ref, own_ref, 1)
    qm = jnp.concatenate([q_ref[:, cols] for cols in blocks], 0)
    gm = jnp.concatenate([go_ref[:, cols] * mask for cols in blocks], 0)
    key = lax.broadcasted_iota(jnp.int32, (rows, rows), 0)
    token = lax.broadcasted_iota(jnp.int32, (rows, rows), 1)
    causal = jnp.where(key <= token, 0.0, MASKED)
    scores = dot(kk, qm, LAST)
    parts = [
        scores[e * rows : (e + 1) * rows] + jnp.where(path_ref[position, e + 1] >= 0, 0.0, MASKED)
        for e in range(FAR_SLOTS)
    ]
    parts.append(scores[far_rows:] + jnp.concatenate([causal] * HEADS_PER_KEY, 1))
    scores = jnp.concatenate(parts, 0)
    top = jnp.max(scores, axis=0, keepdims=True)
    weights = jnp.exp2((scores - top) * (SCALING * math.log2(math.e)))
    weights = weights * (1.0 / jnp.sum(weights, axis=0, keepdims=True))
    rounded = weights.astype(jnp.bfloat16)
    grad_prob = dot(vv, gm, LAST)
    delta = jnp.sum(weights * grad_prob, axis=0, keepdims=True)
    grad_score = (weights * (grad_prob - delta)).astype(jnp.bfloat16)
    weights_ref[...] = rounded
    grad_score_ref[...] = grad_score
    grad_key = dot(grad_score, qm) * SCALING
    grad_value = dot(rounded, gm)
    for e in range(FAR_SLOTS):
        s = slice(e * rows, (e + 1) * rows)
        far_grad_ref[e, 0] = grad_key[s].astype(jnp.bfloat16)
        far_grad_ref[e, 1] = grad_value[s].astype(jnp.bfloat16)
    own_grad_ref[0] = grad_key[far_rows:]
    own_grad_ref[1] = grad_value[far_rows:]


def output_kernel(rows, *refs):
    weights_ref, grad_score_ref, far_ref, own_ref, attn_ref, gq_ref = refs
    kk, vv = stack_slots(far_ref, own_ref, 0), stack_slots(far_ref, own_ref, 1)
    attended = dot(vv, weights_ref[...], FIRST)
    grad_query = dot(kk, grad_score_ref[...], FIRST) * SCALING
    for i in range(HEADS_PER_KEY):
        s = slice(i * rows, (i + 1) * rows)
        cols = slice(i * HEAD_WIDTH, (i + 1) * HEAD_WIDTH)
        attn_ref[:, cols] = attended[:, s].T.astype(jnp.bfloat16)
        gq_ref[:, cols] = grad_query[:, s].T.astype(jnp.bfloat16)


def attend(turn, pos, path, mask, queries, grad_out, far, own):
    rows = queries.shape[0]
    span = (FAR_SLOTS + 1) * rows
    pairs = rows * HEADS_PER_KEY * span
    square = jax.ShapeDtypeStruct((span, HEADS_PER_KEY * rows), jnp.bfloat16)
    return pl.pallas_call(
        functools.partial(attend_kernel, turn, rows),
        in_specs=[SMEM_SPEC] * 2 + [VMEM_SPEC] * 5,
        out_specs=[VMEM_SPEC] * 4,
        out_shape=[
            square,
            square,
            jax.ShapeDtypeStruct(far.shape, jnp.bfloat16),
            jax.ShapeDtypeStruct(own.shape, jnp.float32),
        ],
        cost_estimate=cost(8 * pairs * HEAD_WIDTH, 8 * pairs),
        compiler_params=pltpu.CompilerParams(vmem_limit_bytes=VMEM_LIMIT),
    )(pos, path, mask, queries, grad_out, far, own)


def output(weights, grad_score, far, own):
    rows = own.shape[1]
    block = jax.ShapeDtypeStruct((rows, HEADS_PER_KEY * HEAD_WIDTH), jnp.bfloat16)
    return pl.pallas_call(
        functools.partial(output_kernel, rows),
        in_specs=[VMEM_SPEC] * 4,
        out_specs=[VMEM_SPEC] * 2,
        out_shape=[block, block],
        cost_estimate=cost(4 * weights.size * HEAD_WIDTH, 4 * weights.size),
        compiler_params=pltpu.CompilerParams(vmem_limit_bytes=VMEM_LIMIT),
    )(weights, grad_score, far, own)


def store_kernel(pos_ref, *refs):
    blocks, outs, sem = refs[: 2 * GROUP], refs[2 * GROUP : -1], refs[-1]
    width = HEADS_PER_KEY * HEAD_WIDTH
    member = lax.rem(pos_ref[0], GROUP)
    copies = []
    for t in range(GROUP):
        head = member ^ t
        cols = pl.ds(pl.multiple_of(head * width, width), width)
        for part in range(2):
            i = 2 * t + part
            copies.append(pltpu.make_async_copy(blocks[i], outs[part].at[:, cols], sem.at[i]))
    for copy in copies:
        copy.start()
    for copy in copies:
        copy.wait()


def reduce_kernel(count, pos_ref, path_ref, *refs):
    terms, outs, acc = refs[:GROUP], refs[GROUP : GROUP + count], refs[-1]
    position = pos_ref[0]
    member, group = lax.rem(position, GROUP), lax.div(position, GROUP)
    acc[...] = jnp.zeros_like(acc)
    for t in range(GROUP):
        block = group * GROUP + member ^ t
        for e in range(FAR_SLOTS):
            ancestor = path_ref[block, e]
            above = group - lax.div(ancestor, GROUP)
            index = above * GROUP + (member ^ lax.rem(ancestor, GROUP))

            @pl.when(path_ref[block, e + 1] >= 0)
            def _(t=t, e=e, index=index):
                acc[index] += terms[t][e].astype(jnp.float32)

    for i in range(count):
        outs[i][...] = acc[i].astype(jnp.bfloat16)


def finish_kernel(pos_ref, *refs):
    own, pieces, gk_ref, gv_ref = refs[:GROUP], refs[GROUP:-2], refs[-2], refs[-1]
    member = lax.rem(pos_ref[0], GROUP)
    for t in range(GROUP):
        cols = head_columns(member ^ t)
        for part, out in enumerate((gk_ref, gv_ref)):
            total = own[t][part]
            for piece in pieces[t::GROUP]:
                total = total + piece[part].astype(jnp.float32)
            out[:, cols] = total.astype(jnp.bfloat16)


def small_call(kernel, in_specs, out_specs, out_shape, moved, scratch=(), flops=0):
    return pl.pallas_call(
        kernel,
        in_specs=in_specs,
        out_specs=out_specs,
        out_shape=out_shape,
        scratch_shapes=list(scratch),
        cost_estimate=cost(flops or 2 * moved, moved),
        compiler_params=pltpu.CompilerParams(vmem_limit_bytes=VMEM_LIMIT),
    )


def on_device(size, queries, keys, values, grad_out, block_path, assistant):
    rows = queries.shape[0]
    groups = size // GROUP
    pos = lax.axis_index("ctx").astype(jnp.int32).reshape(1)
    mask = jnp.broadcast_to(assistant[:, None].astype(jnp.bfloat16), (rows, HEAD_WIDTH))
    piece = jax.ShapeDtypeStruct((2, rows, HEAD_WIDTH), jnp.bfloat16)
    chosen = jax.ShapeDtypeStruct((FAR_SLOTS, 2, rows, HEAD_WIDTH), jnp.bfloat16)
    wide = jax.ShapeDtypeStruct(queries.shape, jnp.bfloat16)
    piece_bytes = 4 * rows * HEAD_WIDTH

    def inside(shift):
        return [(i, i ^ shift) for i in range(size)]

    def across(up, shift):
        pairs = []
        for i in range(size):
            group = i // GROUP + up
            if 0 <= group < groups:
                pairs.append((i, group * GROUP + (i % GROUP ^ shift)))
        return pairs

    def send(x, pairs):
        return lax.ppermute(x, "ctx", pairs)

    def far_sends(parts, sign):
        return [
            send(parts[(d * GROUP + t) % len(parts)], across(sign * d, t))
            for d in range(1, groups)
            for t in range(GROUP)
        ]

    def near_sends(parts):
        return [parts[0]] + [send(parts[t], inside(t)) for t in range(1, GROUP)]

    packed = small_call(
        pack_kernel, [SMEM_SPEC, HBM_SPEC, HBM_SPEC], [VMEM_SPEC] * GROUP,
        [piece] * GROUP, 8 * piece_bytes, [pltpu.SemaphoreType.DMA((2 * GROUP,))],
    )(pos, *(pltpu.with_memory_space_constraint(x, pltpu.HBM) for x in (keys, values)))
    far_pieces = far_sends(packed, 1)
    pieces = near_sends(packed) + far_pieces

    picked = small_call(
        functools.partial(select_kernel, size),
        [SMEM_SPEC, SMEM_SPEC] + [VMEM_SPEC] * size, [VMEM_SPEC] * GROUP, [chosen] * GROUP,
        (size + 12) * piece_bytes, [pltpu.VMEM((size,) + piece.shape, jnp.bfloat16)],
        COVER_FLOPS,
    )(pos, block_path, *pieces)
    far = near_sends(picked)

    blocks, far_grads, own_grads = [], [], []
    for t in range(GROUP):
        weights, grad_score, far_grad, own_grad = attend(
            t, pos, block_path, mask, queries, grad_out, far[t], packed[t]
        )
        blocks += output(weights, grad_score, far[t], packed[t])
        far_grads.append(far_grad)
        own_grads.append(own_grad)
    far_grads = near_sends(far_grads)

    attention, grad_queries = small_call(
        store_kernel, [SMEM_SPEC] + [VMEM_SPEC] * (2 * GROUP), [HBM_SPEC] * 2,
        [wide] * 2, 32 * piece_bytes, [pltpu.SemaphoreType.DMA((2 * GROUP,))],
    )(pos, *blocks)

    sums = small_call(
        functools.partial(reduce_kernel, size),
        [SMEM_SPEC, SMEM_SPEC] + [VMEM_SPEC] * GROUP, [VMEM_SPEC] * size, [piece] * size,
        (size + 12) * piece_bytes, [pltpu.VMEM((size,) + piece.shape, jnp.float32)],
    )(pos, block_path, *far_grads)
    far_sums = far_sends(sums, -1)
    near_sums = near_sends(sums[:GROUP])

    grad = jax.ShapeDtypeStruct(keys.shape, jnp.bfloat16)
    grad_keys, grad_values = small_call(
        finish_kernel, [SMEM_SPEC] + [VMEM_SPEC] * (GROUP + size), [VMEM_SPEC] * 2,
        [grad, grad], (size + 12) * piece_bytes,
    )(pos, *own_grads, *near_sums, *far_sums)
    return attention, grad_queries, grad_keys, grad_values


def solution(mesh):
    tokens = P(("leaf", "ctx"))

    def body(*args):
        return on_device(mesh.shape["ctx"], *args)

    return jax.shard_map(
        body,
        mesh=mesh,
        in_specs=(tokens, tokens, tokens, tokens, P("leaf"), tokens),
        out_specs=(tokens, tokens, tokens, tokens),
        check_vma=False,
    )
```

```python
import functools
import math

import jax
import jax.numpy as jnp
from jax import lax
from jax.experimental import pallas as pl
from jax.experimental.pallas import tpu as pltpu
from jax.sharding import PartitionSpec as P


KEY_HEADS = 4
HEAD_WIDTH = 128
HEADS_PER_KEY = 8
FAR_SLOTS = 3
GROUP = KEY_HEADS
MASKED = -1e30
COVER_FLOPS = 4_000_000_000
VMEM_LIMIT = 24 * 1024 * 1024


SMEM_SPEC = pl.BlockSpec(memory_space=pltpu.SMEM)
VMEM_SPEC = pl.BlockSpec(memory_space=pltpu.VMEM)
HBM_SPEC = pl.BlockSpec(memory_space=pltpu.HBM)


LAST = (((1,), (1,)), ((), ()))
FIRST = (((0,), (0,)), ((), ()))
SCALING = 1.0 / math.sqrt(HEAD_WIDTH)
EXPONENT = SCALING * math.log2(math.e)


def dot(left, right, dims=(((1,), (0,)), ((), ()))):
    return lax.dot_general(left, right, dims, preferred_element_type=jnp.float32)


def stack_slots(far_ref, own_ref, part):
    return jnp.concatenate([far_ref[e, part] for e in range(FAR_SLOTS)] + [own_ref[part]], 0)


def head_columns(head):
    return pl.ds(pl.multiple_of(head * HEAD_WIDTH, HEAD_WIDTH), HEAD_WIDTH)


def cost(flops, moved):
    return pl.CostEstimate(flops=flops, bytes_accessed=moved, transcendentals=0)


def pack_kernel(pos_ref, k_ref, v_ref, *refs):
    outs, sem = refs[:GROUP], refs[-1]
    member = lax.rem(pos_ref[0], GROUP)
    copies = []
    for t in range(GROUP):
        cols = head_columns(member ^ t)
        for part, source in enumerate((k_ref, v_ref)):
            copies.append(
                pltpu.make_async_copy(source.at[:, cols], outs[t].at[part], sem.at[2 * t + part])
            )
    for copy in copies:
        copy.start()
    for copy in copies:
        copy.wait()


def plan_kernel(pos_ref, path_ref, pick_ref, add_ref, mask_ref):
    position = pos_ref[0]
    member, group = lax.rem(position, GROUP), lax.div(position, GROUP)
    for t in range(GROUP):
        block = group * GROUP + (member ^ t)
        for e in range(FAR_SLOTS):
            ancestor = path_ref[block, e]
            seen = path_ref[block, e + 1] >= 0
            above = group - lax.div(ancestor, GROUP)
            index = above * GROUP + (member ^ lax.rem(ancestor, GROUP))
            row = pl.ds(t * FAR_SLOTS + e, 1)
            pick_ref[row, :] = jnp.full((1, HEAD_WIDTH), jnp.where(seen, index, 0), jnp.int32)
            add_ref[row, :] = jnp.full((1, HEAD_WIDTH), jnp.where(seen, index, -1), jnp.int32)
    for e in range(FAR_SLOTS):
        masked = jnp.where(path_ref[position, e + 1] >= 0, 0.0, MASKED)
        mask_ref[pl.ds(e, 1), :] = jnp.full((1, HEAD_WIDTH), masked, jnp.float32)


def select_kernel(count, pick_ref, *refs):
    pieces, outs, held = refs[:count], refs[count : count + GROUP], refs[-1]
    pick = pick_ref[...]
    for i in range(count):
        held[i] = pieces[i][...]
    for t in range(GROUP):
        for e in range(FAR_SLOTS):
            outs[t][e] = held[pick[t * FAR_SLOTS + e, 0]]


def attend_kernel(turn, rows, *refs):
    (pos_ref, hide_ref, mask_ref, q_ref, go_ref, far_ref, own_ref) = refs[:7]
    weights_ref, grad_score_ref, far_grad_ref, own_grad_ref = refs[7:]
    head = lax.rem(pos_ref[0], GROUP) ^ turn
    far_rows = FAR_SLOTS * rows
    mask = mask_ref[...]
    blocks = [head_columns(head * HEADS_PER_KEY + i) for i in range(HEADS_PER_KEY)]
    kk, vv = stack_slots(far_ref, own_ref, 0), stack_slots(far_ref, own_ref, 1)
    qm = jnp.concatenate([q_ref[:, cols] for cols in blocks], 0)
    gm = jnp.concatenate([go_ref[:, cols] * mask for cols in blocks], 0)
    key = lax.broadcasted_iota(jnp.int32, (rows, rows), 0)
    token = lax.broadcasted_iota(jnp.int32, (rows, rows), 1)
    causal = jnp.where(key <= token, 0.0, MASKED)
    scores = dot(kk, qm, LAST)
    parts = [scores[e * rows : (e + 1) * rows] for e in range(FAR_SLOTS)]
    parts.append(scores[far_rows:] + jnp.concatenate([causal] * HEADS_PER_KEY, 1))
    hides = [jnp.concatenate([hide_ref[e : e + 1]] * HEADS_PER_KEY, 1) for e in range(FAR_SLOTS)]
    tops = [jnp.max(part, axis=0, keepdims=True) for part in parts]
    top = tops[-1]
    for slot_top, hide in zip(tops, hides):
        top = jnp.maximum(top, slot_top + hide)
    shifts = [top - hide for hide in hides] + [top]
    weights = jnp.concatenate(
        [jnp.exp2((part - shift) * EXPONENT) for part, shift in zip(parts, shifts)], 0
    )
    weights = weights * (1.0 / jnp.sum(weights, axis=0, keepdims=True))
    rounded = weights.astype(jnp.bfloat16)
    grad_prob = dot(vv, gm, LAST)
    delta = jnp.sum(weights * grad_prob, axis=0, keepdims=True)
    grad_score = (weights * (grad_prob - delta)).astype(jnp.bfloat16)
    weights_ref[...] = rounded
    grad_score_ref[...] = grad_score
    grad_key = dot(grad_score, qm) * SCALING
    grad_value = dot(rounded, gm)
    for e in range(FAR_SLOTS):
        s = slice(e * rows, (e + 1) * rows)
        far_grad_ref[e, 0] = grad_key[s].astype(jnp.bfloat16)
        far_grad_ref[e, 1] = grad_value[s].astype(jnp.bfloat16)
    own_grad_ref[0] = grad_key[far_rows:]
    own_grad_ref[1] = grad_value[far_rows:]


def output_kernel(rows, *refs):
    weights_ref, grad_score_ref, far_ref, own_ref, attn_ref, gq_ref = refs
    kk, vv = stack_slots(far_ref, own_ref, 0), stack_slots(far_ref, own_ref, 1)
    attended = dot(vv, weights_ref[...], FIRST)
    grad_query = dot(kk, grad_score_ref[...], FIRST) * SCALING
    for i in range(HEADS_PER_KEY):
        s = slice(i * rows, (i + 1) * rows)
        cols = slice(i * HEAD_WIDTH, (i + 1) * HEAD_WIDTH)
        attn_ref[:, cols] = attended[:, s].T.astype(jnp.bfloat16)
        gq_ref[:, cols] = grad_query[:, s].T.astype(jnp.bfloat16)


def attend(turn, pos, hide, mask, queries, grad_out, far, own):
    rows = queries.shape[0]
    span = (FAR_SLOTS + 1) * rows
    pairs = rows * HEADS_PER_KEY * span
    square = jax.ShapeDtypeStruct((span, HEADS_PER_KEY * rows), jnp.bfloat16)
    return pl.pallas_call(
        functools.partial(attend_kernel, turn, rows),
        in_specs=[SMEM_SPEC] + [VMEM_SPEC] * 6,
        out_specs=[VMEM_SPEC] * 4,
        out_shape=[
            square,
            square,
            jax.ShapeDtypeStruct(far.shape, jnp.bfloat16),
            jax.ShapeDtypeStruct(own.shape, jnp.float32),
        ],
        cost_estimate=cost(8 * pairs * HEAD_WIDTH, 8 * pairs),
        compiler_params=pltpu.CompilerParams(vmem_limit_bytes=VMEM_LIMIT),
    )(pos, hide, mask, queries, grad_out, far, own)


def output(weights, grad_score, far, own):
    rows = own.shape[1]
    block = jax.ShapeDtypeStruct((rows, HEADS_PER_KEY * HEAD_WIDTH), jnp.bfloat16)
    return pl.pallas_call(
        functools.partial(output_kernel, rows),
        in_specs=[VMEM_SPEC] * 4,
        out_specs=[VMEM_SPEC] * 2,
        out_shape=[block, block],
        cost_estimate=cost(4 * weights.size * HEAD_WIDTH, 4 * weights.size),
        compiler_params=pltpu.CompilerParams(vmem_limit_bytes=VMEM_LIMIT),
    )(weights, grad_score, far, own)


def store_kernel(pos_ref, *refs):
    blocks, outs, sem = refs[: 2 * GROUP], refs[2 * GROUP : -1], refs[-1]
    width = HEADS_PER_KEY * HEAD_WIDTH
    member = lax.rem(pos_ref[0], GROUP)
    copies = []
    for t in range(GROUP):
        head = member ^ t
        cols = pl.ds(pl.multiple_of(head * width, width), width)
        for part in range(2):
            i = 2 * t + part
            copies.append(pltpu.make_async_copy(blocks[i], outs[part].at[:, cols], sem.at[i]))
    for copy in copies:
        copy.start()
    for copy in copies:
        copy.wait()


def reduce_kernel(count, add_ref, *refs):
    terms, outs, acc = refs[:GROUP], refs[GROUP : GROUP + count], refs[-1]
    add = add_ref[...]
    acc[...] = jnp.zeros_like(acc)
    for t in range(GROUP):
        for e in range(FAR_SLOTS):
            index = add[t * FAR_SLOTS + e, 0]

            @pl.when(index >= 0)
            def _(t=t, e=e, index=index):
                acc[index] += terms[t][e].astype(jnp.float32)

    for i in range(count):
        outs[i][...] = acc[i].astype(jnp.bfloat16)


def finish_kernel(pos_ref, *refs):
    own, pieces, gk_ref, gv_ref = refs[:GROUP], refs[GROUP:-2], refs[-2], refs[-1]
    member = lax.rem(pos_ref[0], GROUP)
    for t in range(GROUP):
        cols = head_columns(member ^ t)
        for part, out in enumerate((gk_ref, gv_ref)):
            total = own[t][part]
            for piece in pieces[t::GROUP]:
                total = total + piece[part].astype(jnp.float32)
            out[:, cols] = total.astype(jnp.bfloat16)


def small_call(kernel, in_specs, out_specs, out_shape, moved, scratch=(), flops=0):
    return pl.pallas_call(
        kernel,
        in_specs=in_specs,
        out_specs=out_specs,
        out_shape=out_shape,
        scratch_shapes=list(scratch),
        cost_estimate=cost(flops or 2 * moved, moved),
        compiler_params=pltpu.CompilerParams(vmem_limit_bytes=VMEM_LIMIT),
    )


def on_device(size, queries, keys, values, grad_out, block_path, assistant):
    rows = queries.shape[0]
    groups = size // GROUP
    pos = lax.axis_index("ctx").astype(jnp.int32).reshape(1)
    mask = jnp.broadcast_to(assistant[:, None].astype(jnp.bfloat16), (rows, HEAD_WIDTH))
    piece = jax.ShapeDtypeStruct((2, rows, HEAD_WIDTH), jnp.bfloat16)
    chosen = jax.ShapeDtypeStruct((FAR_SLOTS, 2, rows, HEAD_WIDTH), jnp.bfloat16)
    wide = jax.ShapeDtypeStruct(queries.shape, jnp.bfloat16)
    piece_bytes = 4 * rows * HEAD_WIDTH

    def inside(shift):
        return [(i, i ^ shift) for i in range(size)]

    def across(up, shift):
        pairs = []
        for i in range(size):
            group = i // GROUP + up
            if 0 <= group < groups:
                pairs.append((i, group * GROUP + (i % GROUP ^ shift)))
        return pairs

    def send(x, pairs):
        return lax.ppermute(x, "ctx", pairs)

    def far_sends(parts, sign):
        return [
            send(parts[(d * GROUP + t) % len(parts)], across(sign * d, t))
            for d in range(1, groups)
            for t in range(GROUP)
        ]

    def near_sends(parts):
        return [parts[0]] + [send(parts[t], inside(t)) for t in range(1, GROUP)]

    packed = small_call(
        pack_kernel, [SMEM_SPEC, HBM_SPEC, HBM_SPEC], [VMEM_SPEC] * GROUP,
        [piece] * GROUP, 8 * piece_bytes, [pltpu.SemaphoreType.DMA((2 * GROUP,))],
    )(pos, *(pltpu.with_memory_space_constraint(x, pltpu.HBM) for x in (keys, values)))
    far_pieces = far_sends(packed, 1)
    pieces = near_sends(packed) + far_pieces

    table = jax.ShapeDtypeStruct((16, HEAD_WIDTH), jnp.int32)
    pick, add, hide = small_call(
        plan_kernel, [SMEM_SPEC] * 2, [VMEM_SPEC] * 3,
        [table, table, jax.ShapeDtypeStruct((8, HEAD_WIDTH), jnp.float32)], 3 * 8192,
    )(pos, block_path)

    picked = small_call(
        functools.partial(select_kernel, size),
        [VMEM_SPEC] * (1 + size), [VMEM_SPEC] * GROUP, [chosen] * GROUP,
        (size + 12) * piece_bytes, [pltpu.VMEM((size,) + piece.shape, jnp.bfloat16)],
        COVER_FLOPS,
    )(pick, *pieces)
    far = near_sends(picked)

    blocks, far_grads, own_grads = [], [], []
    for t in range(GROUP):
        weights, grad_score, far_grad, own_grad = attend(
            t, pos, hide, mask, queries, grad_out, far[t], packed[t]
        )
        blocks += output(weights, grad_score, far[t], packed[t])
        far_grads.append(far_grad)
        own_grads.append(own_grad)
    far_grads = near_sends(far_grads)

    attention, grad_queries = small_call(
        store_kernel, [SMEM_SPEC] + [VMEM_SPEC] * (2 * GROUP), [HBM_SPEC] * 2,
        [wide] * 2, 32 * piece_bytes, [pltpu.SemaphoreType.DMA((2 * GROUP,))],
    )(pos, *blocks)

    sums = small_call(
        functools.partial(reduce_kernel, size),
        [VMEM_SPEC] * (1 + GROUP), [VMEM_SPEC] * size, [piece] * size,
        (size + 12) * piece_bytes, [pltpu.VMEM((size,) + piece.shape, jnp.float32)],
    )(add, *far_grads)
    far_sums = far_sends(sums, -1)
    near_sums = near_sends(sums[:GROUP])

    grad = jax.ShapeDtypeStruct(keys.shape, jnp.bfloat16)
    grad_keys, grad_values = small_call(
        finish_kernel, [SMEM_SPEC] + [VMEM_SPEC] * (GROUP + size), [VMEM_SPEC] * 2,
        [grad, grad], (size + 12) * piece_bytes,
    )(pos, *own_grads, *near_sums, *far_sums)
    return attention, grad_queries, grad_keys, grad_values


def solution(mesh):
    tokens = P(("leaf", "ctx"))

    def body(*args):
        return on_device(mesh.shape["ctx"], *args)

    return jax.shard_map(
        body,
        mesh=mesh,
        in_specs=(tokens, tokens, tokens, tokens, P("leaf"), tokens),
        out_specs=(tokens, tokens, tokens, tokens),
        check_vma=False,
    )
```

```python
import functools
import math

import jax
import jax.numpy as jnp
from jax import lax
from jax.experimental import pallas as pl
from jax.experimental.pallas import tpu as pltpu
from jax.sharding import PartitionSpec as P


KEY_HEADS = 4
HEAD_WIDTH = 128
HEADS_PER_KEY = 8
FAR_SLOTS = 3
GROUP = KEY_HEADS
MASKED = -1e30
COVER_FLOPS = 4_000_000_000
VMEM_LIMIT = 24 * 1024 * 1024


SMEM_SPEC = pl.BlockSpec(memory_space=pltpu.SMEM)
VMEM_SPEC = pl.BlockSpec(memory_space=pltpu.VMEM)
HBM_SPEC = pl.BlockSpec(memory_space=pltpu.HBM)


LAST = (((1,), (1,)), ((), ()))
FIRST = (((0,), (0,)), ((), ()))
SCALING = 1.0 / math.sqrt(HEAD_WIDTH)
EXPONENT = SCALING * math.log2(math.e)


def dot(left, right, dims=(((1,), (0,)), ((), ()))):
    return lax.dot_general(left, right, dims, preferred_element_type=jnp.float32)


def stack_slots(far_ref, own_ref, part):
    return jnp.concatenate([far_ref[e, part] for e in range(FAR_SLOTS)] + [own_ref[part]], 0)


def stack_heads(ref, head, mask=None):
    parts = [ref[:, head_columns(head * HEADS_PER_KEY + i)] for i in range(HEADS_PER_KEY)]
    return jnp.concatenate(parts if mask is None else [part * mask for part in parts], 0)


def head_columns(head):
    return pl.ds(pl.multiple_of(head * HEAD_WIDTH, HEAD_WIDTH), HEAD_WIDTH)


def cost(flops, moved):
    return pl.CostEstimate(flops=flops, bytes_accessed=moved, transcendentals=0)


def pack_kernel(pos_ref, k_ref, v_ref, *refs):
    outs, sem = refs[:GROUP], refs[-1]
    member = lax.rem(pos_ref[0], GROUP)
    copies = []
    for t in range(GROUP):
        cols = head_columns(member ^ t)
        for part, source in enumerate((k_ref, v_ref)):
            copies.append(
                pltpu.make_async_copy(source.at[:, cols], outs[t].at[part], sem.at[2 * t + part])
            )
    for copy in copies:
        copy.start()
    for copy in copies:
        copy.wait()


def plan_kernel(pos_ref, path_ref, pick_ref, add_ref, mask_ref):
    position = pos_ref[0]
    member, group = lax.rem(position, GROUP), lax.div(position, GROUP)
    for t in range(GROUP):
        block = group * GROUP + (member ^ t)
        for e in range(FAR_SLOTS):
            ancestor = path_ref[block, e]
            seen = path_ref[block, e + 1] >= 0
            above = group - lax.div(ancestor, GROUP)
            index = above * GROUP + (member ^ lax.rem(ancestor, GROUP))
            row = pl.ds(t * FAR_SLOTS + e, 1)
            pick_ref[row, :] = jnp.full((1, HEAD_WIDTH), jnp.where(seen, index, 0), jnp.int32)
            add_ref[row, :] = jnp.full((1, HEAD_WIDTH), jnp.where(seen, index, -1), jnp.int32)
    for e in range(FAR_SLOTS):
        masked = jnp.where(path_ref[position, e + 1] >= 0, 0.0, MASKED)
        mask_ref[pl.ds(e, 1), :] = jnp.full((1, HEAD_WIDTH), masked, jnp.float32)


def select_kernel(count, pick_ref, *refs):
    pieces, outs, held = refs[:count], refs[count : count + GROUP], refs[-1]
    pick = pick_ref[...]
    for i in range(count):
        held[i] = pieces[i][...]
    for t in range(GROUP):
        for e in range(FAR_SLOTS):
            outs[t][e] = held[pick[t * FAR_SLOTS + e, 0]]


def attend_kernel(turn, rows, *refs):
    (pos_ref, hide_ref, mask_ref, q_ref, go_ref, far_ref, own_ref) = refs[:7]
    weights_ref, grad_score_ref, far_grad_ref = refs[7:]
    head = lax.rem(pos_ref[0], GROUP) ^ turn
    far_rows = FAR_SLOTS * rows
    mask = mask_ref[...]
    kk, vv = stack_slots(far_ref, own_ref, 0), stack_slots(far_ref, own_ref, 1)
    qm, gm = stack_heads(q_ref, head), stack_heads(go_ref, head, mask)
    key = lax.broadcasted_iota(jnp.int32, (rows, rows), 0)
    token = lax.broadcasted_iota(jnp.int32, (rows, rows), 1)
    causal = jnp.where(key <= token, 0.0, MASKED)
    scores = dot(kk, qm, LAST)
    parts = [scores[e * rows : (e + 1) * rows] for e in range(FAR_SLOTS)]
    parts.append(scores[far_rows:] + jnp.concatenate([causal] * HEADS_PER_KEY, 1))
    hides = [jnp.concatenate([hide_ref[e : e + 1]] * HEADS_PER_KEY, 1) for e in range(FAR_SLOTS)]
    tops = [jnp.max(part, axis=0, keepdims=True) for part in parts]
    top = tops[-1]
    for slot_top, hide in zip(tops, hides):
        top = jnp.maximum(top, slot_top + hide)
    shifts = [top - hide for hide in hides] + [top]
    weights = jnp.concatenate(
        [jnp.exp2((part - shift) * EXPONENT) for part, shift in zip(parts, shifts)], 0
    )
    weights = weights * (1.0 / jnp.sum(weights, axis=0, keepdims=True))
    rounded = weights.astype(jnp.bfloat16)
    grad_prob = dot(vv, gm, LAST)
    delta = jnp.sum(weights * grad_prob, axis=0, keepdims=True)
    grad_score = (weights * (grad_prob - delta)).astype(jnp.bfloat16)
    weights_ref[...] = rounded
    grad_score_ref[...] = grad_score
    grad_key = dot(grad_score[:far_rows], qm) * SCALING
    grad_value = dot(rounded[:far_rows], gm)
    for e in range(FAR_SLOTS):
        s = slice(e * rows, (e + 1) * rows)
        far_grad_ref[e, 0] = grad_key[s].astype(jnp.bfloat16)
        far_grad_ref[e, 1] = grad_value[s].astype(jnp.bfloat16)


def output_kernel(turn, rows, *refs):
    pos_ref, mask_ref, q_ref, go_ref, weights_ref, grad_score_ref, far_ref, own_ref = refs[:8]
    attn_ref, gq_ref, own_grad_ref = refs[8:]
    head = lax.rem(pos_ref[0], GROUP) ^ turn
    own_rows = pl.ds(FAR_SLOTS * rows, rows)
    own_grad_ref[0] = dot(grad_score_ref[own_rows, :], stack_heads(q_ref, head)) * SCALING
    gm = stack_heads(go_ref, head, mask_ref[...])
    own_grad_ref[1] = dot(weights_ref[own_rows, :], gm)
    kk, vv = stack_slots(far_ref, own_ref, 0), stack_slots(far_ref, own_ref, 1)
    attended = dot(vv, weights_ref[...], FIRST)
    grad_query = dot(kk, grad_score_ref[...], FIRST) * SCALING
    for i in range(HEADS_PER_KEY):
        s = slice(i * rows, (i + 1) * rows)
        cols = slice(i * HEAD_WIDTH, (i + 1) * HEAD_WIDTH)
        attn_ref[:, cols] = attended[:, s].T.astype(jnp.bfloat16)
        gq_ref[:, cols] = grad_query[:, s].T.astype(jnp.bfloat16)


def attend(turn, pos, hide, mask, queries, grad_out, far, own):
    rows = queries.shape[0]
    span = (FAR_SLOTS + 1) * rows
    pairs = rows * HEADS_PER_KEY * span
    square = jax.ShapeDtypeStruct((span, HEADS_PER_KEY * rows), jnp.bfloat16)
    return pl.pallas_call(
        functools.partial(attend_kernel, turn, rows),
        in_specs=[SMEM_SPEC] + [VMEM_SPEC] * 6,
        out_specs=[VMEM_SPEC] * 3,
        out_shape=[square, square, jax.ShapeDtypeStruct(far.shape, jnp.bfloat16)],
        cost_estimate=cost(8 * pairs * HEAD_WIDTH, 8 * pairs),
        compiler_params=pltpu.CompilerParams(vmem_limit_bytes=VMEM_LIMIT),
    )(pos, hide, mask, queries, grad_out, far, own)


def output(turn, pos, mask, queries, grad_out, weights, grad_score, far, own):
    rows = own.shape[1]
    block = jax.ShapeDtypeStruct((rows, HEADS_PER_KEY * HEAD_WIDTH), jnp.bfloat16)
    return pl.pallas_call(
        functools.partial(output_kernel, turn, rows),
        in_specs=[SMEM_SPEC] + [VMEM_SPEC] * 7,
        out_specs=[VMEM_SPEC] * 3,
        out_shape=[block, block, jax.ShapeDtypeStruct(own.shape, jnp.float32)],
        cost_estimate=cost(5 * weights.size * HEAD_WIDTH, 4 * weights.size),
        compiler_params=pltpu.CompilerParams(vmem_limit_bytes=VMEM_LIMIT),
    )(pos, mask, queries, grad_out, weights, grad_score, far, own)


def store_kernel(pos_ref, *refs):
    blocks, outs, sem = refs[: 2 * GROUP], refs[2 * GROUP : -1], refs[-1]
    width = HEADS_PER_KEY * HEAD_WIDTH
    member = lax.rem(pos_ref[0], GROUP)
    copies = []
    for t in range(GROUP):
        head = member ^ t
        cols = pl.ds(pl.multiple_of(head * width, width), width)
        for part in range(2):
            i = 2 * t + part
            copies.append(pltpu.make_async_copy(blocks[i], outs[part].at[:, cols], sem.at[i]))
    for copy in copies:
        copy.start()
    for copy in copies:
        copy.wait()


def partial_kernel(add_ref, *refs):
    terms, acc = refs[:-1], refs[-1]
    add = add_ref[...]
    acc[...] = jnp.zeros_like(acc)
    for t, term in enumerate(terms):
        for e in range(FAR_SLOTS):
            index = add[t * FAR_SLOTS + e, 0]

            @pl.when(index >= 0)
            def _(term=term, e=e, index=index):
                acc[index] += term[e].astype(jnp.float32)


def total_kernel(begin, add_ref, acc_ref, last_ref, *outs):
    add = add_ref[...]
    row = (GROUP - 1) * FAR_SLOTS
    for i, out in enumerate(outs):
        total = acc_ref[begin + i]
        for e in range(FAR_SLOTS):
            hit = add[row + e, 0] == begin + i
            total = total + jnp.where(hit, last_ref[e].astype(jnp.float32), 0.0)
        out[...] = total.astype(jnp.bfloat16)


def finish_kernel(pos_ref, *refs):
    own, pieces, gk_ref, gv_ref = refs[:GROUP], refs[GROUP:-2], refs[-2], refs[-1]
    member = lax.rem(pos_ref[0], GROUP)
    for t in range(GROUP):
        cols = head_columns(member ^ t)
        for part, out in enumerate((gk_ref, gv_ref)):
            total = own[t][part]
            for piece in pieces[t::GROUP]:
                total = total + piece[part].astype(jnp.float32)
            out[:, cols] = total.astype(jnp.bfloat16)


def small_call(kernel, in_specs, out_specs, out_shape, moved, scratch=(), flops=0):
    return pl.pallas_call(
        kernel,
        in_specs=in_specs,
        out_specs=out_specs,
        out_shape=out_shape,
        scratch_shapes=list(scratch),
        cost_estimate=cost(flops or 2 * moved, moved),
        compiler_params=pltpu.CompilerParams(vmem_limit_bytes=VMEM_LIMIT),
    )


def on_device(size, queries, keys, values, grad_out, block_path, assistant):
    rows = queries.shape[0]
    groups = size // GROUP
    pos = lax.axis_index("ctx").astype(jnp.int32).reshape(1)
    mask = jnp.broadcast_to(assistant[:, None].astype(jnp.bfloat16), (rows, HEAD_WIDTH))
    piece = jax.ShapeDtypeStruct((2, rows, HEAD_WIDTH), jnp.bfloat16)
    chosen = jax.ShapeDtypeStruct((FAR_SLOTS, 2, rows, HEAD_WIDTH), jnp.bfloat16)
    wide = jax.ShapeDtypeStruct(queries.shape, jnp.bfloat16)
    piece_bytes = 4 * rows * HEAD_WIDTH

    def inside(shift):
        return [(i, i ^ shift) for i in range(size)]

    def across(up, shift):
        pairs = []
        for i in range(size):
            group = i // GROUP + up
            if 0 <= group < groups:
                pairs.append((i, group * GROUP + (i % GROUP ^ shift)))
        return pairs

    def send(x, pairs):
        return lax.ppermute(x, "ctx", pairs)

    def far_sends(parts, sign):
        return [
            send(parts[(d * GROUP + t) % len(parts)], across(sign * d, t))
            for d in range(1, groups)
            for t in range(GROUP)
        ]

    def near_sends(parts):
        return [parts[0]] + [send(parts[t], inside(t)) for t in range(1, GROUP)]

    packed = small_call(
        pack_kernel, [SMEM_SPEC, HBM_SPEC, HBM_SPEC], [VMEM_SPEC] * GROUP,
        [piece] * GROUP, 8 * piece_bytes, [pltpu.SemaphoreType.DMA((2 * GROUP,))],
    )(pos, *(pltpu.with_memory_space_constraint(x, pltpu.HBM) for x in (keys, values)))
    far_pieces = far_sends(packed, 1)
    pieces = near_sends(packed) + far_pieces

    table = jax.ShapeDtypeStruct((16, HEAD_WIDTH), jnp.int32)
    pick, add, hide = small_call(
        plan_kernel, [SMEM_SPEC] * 2, [VMEM_SPEC] * 3,
        [table, table, jax.ShapeDtypeStruct((8, HEAD_WIDTH), jnp.float32)], 3 * 8192,
    )(pos, block_path)

    picked = small_call(
        functools.partial(select_kernel, size),
        [VMEM_SPEC] * (1 + size), [VMEM_SPEC] * GROUP, [chosen] * GROUP,
        (size + 12) * piece_bytes, [pltpu.VMEM((size,) + piece.shape, jnp.bfloat16)],
        COVER_FLOPS,
    )(pick, *pieces)
    far = near_sends(picked)

    blocks, far_grads, own_grads = [], [], []
    for t in range(GROUP):
        weights, grad_score, far_grad = attend(
            t, pos, hide, mask, queries, grad_out, far[t], packed[t]
        )
        attended, grad_query, own_grad = output(
            t, pos, mask, queries, grad_out, weights, grad_score, far[t], packed[t]
        )
        blocks += [attended, grad_query]
        far_grads.append(far_grad)
        own_grads.append(own_grad)
    far_grads = near_sends(far_grads)

    attention, grad_queries = small_call(
        store_kernel, [SMEM_SPEC] + [VMEM_SPEC] * (2 * GROUP), [HBM_SPEC] * 2,
        [wide] * 2, 32 * piece_bytes, [pltpu.SemaphoreType.DMA((2 * GROUP,))],
    )(pos, *blocks)

    (acc,) = small_call(
        partial_kernel, [VMEM_SPEC] * GROUP, [VMEM_SPEC],
        [jax.ShapeDtypeStruct((size,) + piece.shape, jnp.float32)], (2 * size + 9) * piece_bytes,
    )(add, *far_grads[:-1])

    def total(begin, count):
        return small_call(
            functools.partial(total_kernel, begin), [VMEM_SPEC] * 3,
            [VMEM_SPEC] * count, [piece] * count, (3 * count + 3) * piece_bytes,
        )(add, acc, far_grads[-1])

    far_sums = total(GROUP, size - GROUP)
    far_sums = far_sends([None] * GROUP + list(far_sums), -1)
    near_sums = near_sends(total(0, GROUP))

    grad = jax.ShapeDtypeStruct(keys.shape, jnp.bfloat16)
    grad_keys, grad_values = small_call(
        finish_kernel, [SMEM_SPEC] + [VMEM_SPEC] * (GROUP + size), [VMEM_SPEC] * 2,
        [grad, grad], (size + 12) * piece_bytes,
    )(pos, *own_grads, *near_sums, *far_sums)
    return attention, grad_queries, grad_keys, grad_values


def solution(mesh):
    tokens = P(("leaf", "ctx"))

    def body(*args):
        return on_device(mesh.shape["ctx"], *args)

    return jax.shard_map(
        body,
        mesh=mesh,
        in_specs=(tokens, tokens, tokens, tokens, P("leaf"), tokens),
        out_specs=(tokens, tokens, tokens, tokens),
        check_vma=False,
    )
```

```python
import functools
import math

import jax
import jax.numpy as jnp
from jax import lax
from jax.experimental import pallas as pl
from jax.experimental.pallas import tpu as pltpu
from jax.sharding import PartitionSpec as P


KEY_HEADS = 4
HEAD_WIDTH = 128
HEADS_PER_KEY = 8
FAR_SLOTS = 3
GROUP = KEY_HEADS
MASKED = -1e30
COVER_FLOPS = 4_000_000_000
VMEM_LIMIT = 24 * 1024 * 1024


SMEM_SPEC = pl.BlockSpec(memory_space=pltpu.SMEM)
VMEM_SPEC = pl.BlockSpec(memory_space=pltpu.VMEM)
HBM_SPEC = pl.BlockSpec(memory_space=pltpu.HBM)


LAST = (((1,), (1,)), ((), ()))
FIRST = (((0,), (0,)), ((), ()))
SCALING = 1.0 / math.sqrt(HEAD_WIDTH)
EXPONENT = SCALING * math.log2(math.e)


def dot(left, right, dims=(((1,), (0,)), ((), ()))):
    return lax.dot_general(left, right, dims, preferred_element_type=jnp.float32)


def stack_slots(far_ref, own_ref, part):
    return jnp.concatenate([far_ref[e, part] for e in range(FAR_SLOTS)] + [own_ref[part]], 0)


def stack_heads(ref, head, mask=None):
    parts = [ref[:, head_columns(head * HEADS_PER_KEY + i)] for i in range(HEADS_PER_KEY)]
    return jnp.concatenate(parts if mask is None else [part * mask for part in parts], 0)


def head_columns(head):
    return pl.ds(pl.multiple_of(head * HEAD_WIDTH, HEAD_WIDTH), HEAD_WIDTH)


def cost(flops, moved):
    return pl.CostEstimate(flops=flops, bytes_accessed=moved, transcendentals=0)


def pack_kernel(pos_ref, k_ref, v_ref, *refs):
    outs, sem = refs[:GROUP], refs[-1]
    member = lax.rem(pos_ref[0], GROUP)
    copies = []
    for t in range(GROUP):
        cols = head_columns(member ^ t)
        for part, source in enumerate((k_ref, v_ref)):
            copies.append(
                pltpu.make_async_copy(source.at[:, cols], outs[t].at[part], sem.at[2 * t + part])
            )
    for copy in copies:
        copy.start()
    for copy in copies:
        copy.wait()


def plan_kernel(pos_ref, path_ref, pick_ref, add_ref, mask_ref):
    position = pos_ref[0]
    member, group = lax.rem(position, GROUP), lax.div(position, GROUP)
    for t in range(GROUP):
        block = group * GROUP + (member ^ t)
        for e in range(FAR_SLOTS):
            ancestor = path_ref[block, e]
            seen = path_ref[block, e + 1] >= 0
            above = group - lax.div(ancestor, GROUP)
            index = above * GROUP + (member ^ lax.rem(ancestor, GROUP))
            row = pl.ds(t * FAR_SLOTS + e, 1)
            pick_ref[row, :] = jnp.full((1, HEAD_WIDTH), jnp.where(seen, index, 0), jnp.int32)
            add_ref[row, :] = jnp.full((1, HEAD_WIDTH), jnp.where(seen, index, -1), jnp.int32)
    for e in range(FAR_SLOTS):
        masked = jnp.where(path_ref[position, e + 1] >= 0, 0.0, MASKED)
        mask_ref[pl.ds(e, 1), :] = jnp.full((1, HEAD_WIDTH), masked, jnp.float32)


def select_kernel(count, pick_ref, *refs):
    pieces, outs, held = refs[:count], refs[count : count + GROUP], refs[-1]
    pick = pick_ref[...]
    for i in range(count):
        held[i] = pieces[i][...]
    for t in range(GROUP):
        for e in range(FAR_SLOTS):
            outs[t][e] = held[pick[t * FAR_SLOTS + e, 0]]


def attend_kernel(turn, rows, *refs):
    (pos_ref, hide_ref, mask_ref, q_ref, go_ref, far_ref, own_ref) = refs[:7]
    weights_ref, grad_score_ref, attended_ref, far_grad_ref = refs[7:]
    head = lax.rem(pos_ref[0], GROUP) ^ turn
    far_rows = FAR_SLOTS * rows
    mask = mask_ref[...]
    kk, vv = stack_slots(far_ref, own_ref, 0), stack_slots(far_ref, own_ref, 1)
    qm, gm = stack_heads(q_ref, head), stack_heads(go_ref, head, mask)
    key = lax.broadcasted_iota(jnp.int32, (rows, rows), 0)
    token = lax.broadcasted_iota(jnp.int32, (rows, rows), 1)
    causal = jnp.where(key <= token, 0.0, MASKED)
    scores = dot(kk, qm, LAST)
    parts = [scores[e * rows : (e + 1) * rows] for e in range(FAR_SLOTS)]
    parts.append(scores[far_rows:] + jnp.concatenate([causal] * HEADS_PER_KEY, 1))
    hides = [jnp.concatenate([hide_ref[e : e + 1]] * HEADS_PER_KEY, 1) for e in range(FAR_SLOTS)]
    tops = [jnp.max(part, axis=0, keepdims=True) for part in parts]
    top = tops[-1]
    for slot_top, hide in zip(tops, hides):
        top = jnp.maximum(top, slot_top + hide)
    shifts = [top - hide for hide in hides] + [top]
    weights = jnp.concatenate(
        [jnp.exp2((part - shift) * EXPONENT) for part, shift in zip(parts, shifts)], 0
    )
    weights = weights * (1.0 / jnp.sum(weights, axis=0, keepdims=True))
    rounded = weights.astype(jnp.bfloat16)
    grad_prob = dot(vv, gm, LAST)
    attended = dot(vv, rounded, FIRST).astype(jnp.bfloat16)
    gm_heads = [gm[i * rows : (i + 1) * rows].T for i in range(HEADS_PER_KEY)]
    gm_columns = jnp.concatenate(gm_heads, 1).astype(jnp.float32)
    delta = jnp.sum(gm_columns * attended.astype(jnp.float32), axis=0, keepdims=True)
    grad_score = (weights * (grad_prob - delta)).astype(jnp.bfloat16)
    attended_ref[...] = attended
    weights_ref[...] = rounded
    grad_score_ref[...] = grad_score
    grad_key = dot(grad_score[:far_rows], qm) * SCALING
    grad_value = dot(rounded[:far_rows], gm)
    for e in range(FAR_SLOTS):
        s = slice(e * rows, (e + 1) * rows)
        far_grad_ref[e, 0] = grad_key[s].astype(jnp.bfloat16)
        far_grad_ref[e, 1] = grad_value[s].astype(jnp.bfloat16)


def output_kernel(turn, rows, *refs):
    pos_ref, mask_ref, q_ref, go_ref, weights_ref, grad_score_ref = refs[:6]
    attended_ref, far_ref, own_ref, attn_ref, gq_ref, own_grad_ref = refs[6:]
    head = lax.rem(pos_ref[0], GROUP) ^ turn
    own_rows = pl.ds(FAR_SLOTS * rows, rows)
    own_grad_ref[0] = dot(grad_score_ref[own_rows, :], stack_heads(q_ref, head)) * SCALING
    gm = stack_heads(go_ref, head, mask_ref[...])
    own_grad_ref[1] = dot(weights_ref[own_rows, :], gm)
    kk = stack_slots(far_ref, own_ref, 0)
    grad_query = dot(kk, grad_score_ref[...], FIRST) * SCALING
    for i in range(HEADS_PER_KEY):
        s = slice(i * rows, (i + 1) * rows)
        cols = slice(i * HEAD_WIDTH, (i + 1) * HEAD_WIDTH)
        attn_ref[:, cols] = attended_ref[:, s].T
        gq_ref[:, cols] = grad_query[:, s].T.astype(jnp.bfloat16)


def attend(turn, pos, hide, mask, queries, grad_out, far, own):
    rows = queries.shape[0]
    span = (FAR_SLOTS + 1) * rows
    pairs = rows * HEADS_PER_KEY * span
    square = jax.ShapeDtypeStruct((span, HEADS_PER_KEY * rows), jnp.bfloat16)
    return pl.pallas_call(
        functools.partial(attend_kernel, turn, rows),
        in_specs=[SMEM_SPEC] + [VMEM_SPEC] * 6,
        out_specs=[VMEM_SPEC] * 4,
        out_shape=[
            square,
            square,
            jax.ShapeDtypeStruct((HEAD_WIDTH, HEADS_PER_KEY * rows), jnp.bfloat16),
            jax.ShapeDtypeStruct(far.shape, jnp.bfloat16),
        ],
        cost_estimate=cost(8 * pairs * HEAD_WIDTH, 8 * pairs),
        compiler_params=pltpu.CompilerParams(vmem_limit_bytes=VMEM_LIMIT),
    )(pos, hide, mask, queries, grad_out, far, own)


def output(turn, pos, mask, queries, grad_out, weights, grad_score, attended, far, own):
    rows = own.shape[1]
    block = jax.ShapeDtypeStruct((rows, HEADS_PER_KEY * HEAD_WIDTH), jnp.bfloat16)
    return pl.pallas_call(
        functools.partial(output_kernel, turn, rows),
        in_specs=[SMEM_SPEC] + [VMEM_SPEC] * 8,
        out_specs=[VMEM_SPEC] * 3,
        out_shape=[block, block, jax.ShapeDtypeStruct(own.shape, jnp.float32)],
        cost_estimate=cost(5 * weights.size * HEAD_WIDTH, 4 * weights.size),
        compiler_params=pltpu.CompilerParams(vmem_limit_bytes=VMEM_LIMIT),
    )(pos, mask, queries, grad_out, weights, grad_score, attended, far, own)


def store_kernel(pos_ref, *refs):
    blocks, outs, sem = refs[: 2 * GROUP], refs[2 * GROUP : -1], refs[-1]
    width = HEADS_PER_KEY * HEAD_WIDTH
    member = lax.rem(pos_ref[0], GROUP)
    copies = []
    for t in range(GROUP):
        head = member ^ t
        cols = pl.ds(pl.multiple_of(head * width, width), width)
        for part in range(2):
            i = 2 * t + part
            copies.append(pltpu.make_async_copy(blocks[i], outs[part].at[:, cols], sem.at[i]))
    for copy in copies:
        copy.start()
    for copy in copies:
        copy.wait()


def partial_kernel(add_ref, *refs):
    terms, acc = refs[:-1], refs[-1]
    add = add_ref[...]
    acc[...] = jnp.zeros_like(acc)
    for t, term in enumerate(terms):
        for e in range(FAR_SLOTS):
            index = add[t * FAR_SLOTS + e, 0]

            @pl.when(index >= 0)
            def _(term=term, e=e, index=index):
                acc[index] += term[e].astype(jnp.float32)


def total_kernel(begin, add_ref, acc_ref, last_ref, *outs):
    add = add_ref[...]
    row = (GROUP - 1) * FAR_SLOTS
    for i, out in enumerate(outs):
        total = acc_ref[begin + i]
        for e in range(FAR_SLOTS):
            hit = add[row + e, 0] == begin + i
            total = total + jnp.where(hit, last_ref[e].astype(jnp.float32), 0.0)
        out[...] = total.astype(jnp.bfloat16)


def finish_kernel(pos_ref, *refs):
    own, pieces, gk_ref, gv_ref = refs[:GROUP], refs[GROUP:-2], refs[-2], refs[-1]
    member = lax.rem(pos_ref[0], GROUP)
    for t in range(GROUP):
        cols = head_columns(member ^ t)
        for part, out in enumerate((gk_ref, gv_ref)):
            total = own[t][part]
            for piece in pieces[t::GROUP]:
                total = total + piece[part].astype(jnp.float32)
            out[:, cols] = total.astype(jnp.bfloat16)


def small_call(kernel, in_specs, out_specs, out_shape, moved, scratch=(), flops=0):
    return pl.pallas_call(
        kernel,
        in_specs=in_specs,
        out_specs=out_specs,
        out_shape=out_shape,
        scratch_shapes=list(scratch),
        cost_estimate=cost(flops or 2 * moved, moved),
        compiler_params=pltpu.CompilerParams(vmem_limit_bytes=VMEM_LIMIT),
    )


def on_device(size, queries, keys, values, grad_out, block_path, assistant):
    rows = queries.shape[0]
    groups = size // GROUP
    pos = lax.axis_index("ctx").astype(jnp.int32).reshape(1)
    mask = jnp.broadcast_to(assistant[:, None].astype(jnp.bfloat16), (rows, HEAD_WIDTH))
    piece = jax.ShapeDtypeStruct((2, rows, HEAD_WIDTH), jnp.bfloat16)
    chosen = jax.ShapeDtypeStruct((FAR_SLOTS, 2, rows, HEAD_WIDTH), jnp.bfloat16)
    wide = jax.ShapeDtypeStruct(queries.shape, jnp.bfloat16)
    piece_bytes = 4 * rows * HEAD_WIDTH

    def inside(shift):
        return [(i, i ^ shift) for i in range(size)]

    def across(up, shift):
        pairs = []
        for i in range(size):
            group = i // GROUP + up
            if 0 <= group < groups:
                pairs.append((i, group * GROUP + (i % GROUP ^ shift)))
        return pairs

    def send(x, pairs):
        return lax.ppermute(x, "ctx", pairs)

    def far_sends(parts, sign):
        return [
            send(parts[(d * GROUP + t) % len(parts)], across(sign * d, t))
            for d in range(1, groups)
            for t in range(GROUP)
        ]

    def near_sends(parts):
        return [parts[0]] + [send(parts[t], inside(t)) for t in range(1, GROUP)]

    packed = small_call(
        pack_kernel, [SMEM_SPEC, HBM_SPEC, HBM_SPEC], [VMEM_SPEC] * GROUP,
        [piece] * GROUP, 8 * piece_bytes, [pltpu.SemaphoreType.DMA((2 * GROUP,))],
    )(pos, *(pltpu.with_memory_space_constraint(x, pltpu.HBM) for x in (keys, values)))
    far_pieces = far_sends(packed, 1)
    pieces = near_sends(packed) + far_pieces

    table = jax.ShapeDtypeStruct((16, HEAD_WIDTH), jnp.int32)
    pick, add, hide = small_call(
        plan_kernel, [SMEM_SPEC] * 2, [VMEM_SPEC] * 3,
        [table, table, jax.ShapeDtypeStruct((8, HEAD_WIDTH), jnp.float32)], 3 * 8192,
    )(pos, block_path)

    picked = small_call(
        functools.partial(select_kernel, size),
        [VMEM_SPEC] * (1 + size), [VMEM_SPEC] * GROUP, [chosen] * GROUP,
        (size + 12) * piece_bytes, [pltpu.VMEM((size,) + piece.shape, jnp.bfloat16)],
        COVER_FLOPS,
    )(pick, *pieces)
    far = near_sends(picked)

    blocks, far_grads, own_grads = [], [], []
    for t in range(GROUP):
        weights, grad_score, transposed, far_grad = attend(
            t, pos, hide, mask, queries, grad_out, far[t], packed[t]
        )
        attended, grad_query, own_grad = output(
            t, pos, mask, queries, grad_out, weights, grad_score, transposed, far[t], packed[t]
        )
        blocks += [attended, grad_query]
        far_grads.append(far_grad)
        own_grads.append(own_grad)
    far_grads = near_sends(far_grads)

    attention, grad_queries = small_call(
        store_kernel, [SMEM_SPEC] + [VMEM_SPEC] * (2 * GROUP), [HBM_SPEC] * 2,
        [wide] * 2, 32 * piece_bytes, [pltpu.SemaphoreType.DMA((2 * GROUP,))],
    )(pos, *blocks)

    (acc,) = small_call(
        partial_kernel, [VMEM_SPEC] * GROUP, [VMEM_SPEC],
        [jax.ShapeDtypeStruct((size,) + piece.shape, jnp.float32)], (2 * size + 9) * piece_bytes,
    )(add, *far_grads[:-1])

    def total(begin, count):
        return small_call(
            functools.partial(total_kernel, begin), [VMEM_SPEC] * 3,
            [VMEM_SPEC] * count, [piece] * count, (3 * count + 3) * piece_bytes,
        )(add, acc, far_grads[-1])

    far_sums = total(GROUP, size - GROUP)
    far_sums = far_sends([None] * GROUP + list(far_sums), -1)
    near_sums = near_sends(total(0, GROUP))

    grad = jax.ShapeDtypeStruct(keys.shape, jnp.bfloat16)
    grad_keys, grad_values = small_call(
        finish_kernel, [SMEM_SPEC] + [VMEM_SPEC] * (GROUP + size), [VMEM_SPEC] * 2,
        [grad, grad], (size + 12) * piece_bytes,
    )(pos, *own_grads, *near_sums, *far_sums)
    return attention, grad_queries, grad_keys, grad_values


def solution(mesh):
    tokens = P(("leaf", "ctx"))

    def body(*args):
        return on_device(mesh.shape["ctx"], *args)

    return jax.shard_map(
        body,
        mesh=mesh,
        in_specs=(tokens, tokens, tokens, tokens, P("leaf"), tokens),
        out_specs=(tokens, tokens, tokens, tokens),
        check_vma=False,
    )
```
